32 devices in a mesh: elem: 8 (over z, core), lev: 4 (over y, x).
Axes of the slice: x: 2, y: 2, z: 4, core: 2. Of those that a mesh axis runs over, the one named last changes fastest.
Arguments:
- tracers: float32 [512, 16, 640], P('elem', 'lev'), may hold values from 0.1 to 120, as said below
- ref_index: int32 [512, 16], P('elem'), may hold values from 0 to 63
- requests: int32 [8, 2, 16], P('elem'), may hold values from -1 to 63, as said below
- source: int32 [512], P('elem'), may hold values from 0 to 95, as said below
- target_mean: float32 [40], replicated, may hold values from 0.5 to 5
Outputs:
- transported: float32 [512, 16, 640], P('elem', 'lev')
The draws below stay inside these ranges and needn't reach their ends.
Inputs may be any that keep to these rules, and one draw needn't show every extreme that they name: Row 0 of requests[d] holds distinct element indices of block d - 1 (wrapping), row 1 of block d + 1; the valid entries come first and the rest are -1; every row holds 1 to 16 valid entries and some row holds exactly 16. `source`: every slot names an own element (below 64) or a valid entry of the block's requests: 64 + k for row 0, 80 + k for row 1. `tracers`: all entries are positive.
All inputs are finite; a program needn't handle non-finite values.
Results may differ from the reference program's by a relative error of at most 0.0003.
Values sent between devices are 32-bit elements; how exact they have to be, the bound alone decides.
No kernel may reach another device: no remote copies, remote signals or barrier semaphores. Data moves between devices by JAX's collectives and lax.ppermute only.
A program may use at most 64 MiB of HBM per device.

```python
import math
import jax
import jax.numpy as jnp
from jax import lax

TR = 40
NPTS = 16
REFS = 64
ELEM_DEV = 64
SLOTS = 16
NELEM = 512
NLEV = 16
N_ELEM = 8


def routing(key):
    key = jax.random.fold_in(key, 17)
    key_count, key_band, key_busy, key_perm, key_side, key_left, key_right, key_near, key_high = jax.random.split(key, 9)
    low_counts = jax.random.randint(key_count, (N_ELEM, 2), 1, max(SLOTS // 3, 1) + 1)
    high_counts = jax.random.randint(key_high, (N_ELEM, 2), max(SLOTS // 2, 1), SLOTS + 1)
    band_start = jax.random.randint(key_band, (), 0, N_ELEM)
    in_band = (jnp.arange(N_ELEM, dtype=jnp.int32) - band_start) % N_ELEM < max(N_ELEM // 8, 1)
    counts = jnp.where(in_band[:, None], high_counts, low_counts)
    busiest = jax.random.randint(key_busy, (), 0, N_ELEM * 2)
    flat_counts = jnp.where(jnp.arange(N_ELEM * 2, dtype=jnp.int32) == busiest, SLOTS, counts.reshape(-1))
    counts = flat_counts.reshape(N_ELEM, 2)
    row_keys = jax.random.split(key_perm, N_ELEM * 2)

    def choose(one_key):
        return jax.random.permutation(one_key, ELEM_DEV)[:SLOTS]
    element_ids = jax.vmap(choose)(row_keys).reshape(N_ELEM, 2, SLOTS).astype(jnp.int32)
    usable = jnp.arange(SLOTS, dtype=jnp.int32)[None, None, :] < counts[:, :, None]
    requests = jnp.where(usable, element_ids, -1).astype(jnp.int32)
    position = jnp.arange(NELEM, dtype=jnp.int32) % ELEM_DEV
    device = jnp.arange(NELEM, dtype=jnp.int32) // ELEM_DEV
    branch_pick = jax.random.randint(key_side, (NELEM,), 0, 4)
    nearby = jnp.clip(position + jax.random.randint(key_near, (NELEM,), -2, 3), 0, ELEM_DEV - 1)
    left_slot = ELEM_DEV + jax.random.randint(key_left, (NELEM,), 0, counts[device, 0])
    right_slot = ELEM_DEV + SLOTS + jax.random.randint(key_right, (NELEM,), 0, counts[device, 1])
    use_left = (position < ELEM_DEV // 4) & (branch_pick < 2)
    use_right = (position >= ELEM_DEV - ELEM_DEV // 4) & (branch_pick < 2)
    source = jnp.where(use_left, left_slot, jnp.where(use_right, right_slot, nearby)).astype(jnp.int32)
    return (requests, source)


def draw_requests(key, part):
    return routing(key)[0]


def draw_source(key, part):
    return routing(key)[1]


def draw_tracers(key, part):
    key = jax.random.fold_in(key, 29)
    shape = (NELEM, NLEV, TR * NPTS)
    elem_frac = (jnp.arange(NELEM, dtype=jnp.float32) / NELEM)[:, None, None]
    lev_frac = (jnp.arange(NLEV, dtype=jnp.float32) / NLEV)[None, :, None]
    base = jnp.exp(jax.random.uniform(key, shape, jnp.float32, math.log(0.1), math.log(10.0)))
    rising = (1.0 + elem_frac) * (1.0 + 0.5 * lev_frac)
    return (base * rising).astype(jnp.float32)


def plant(values, key, least, top_value):
    spot = [jax.random.randint(jax.random.fold_in(key, axis), (), 0, length) for axis, length in enumerate(values.shape)]
    main_axis = values.shape.index(max(values.shape))
    neighbour = spot[:main_axis] + [(spot[main_axis] + 1) % values.shape[main_axis]] + spot[main_axis + 1:]
    return values.at[tuple(spot)].set(least).at[tuple(neighbour)].set(top_value)


def setup_inputs(seed: int = 0) -> dict:
    arg_keys = jax.random.split(jax.random.key(seed), 6)
    tracers = draw_tracers(jax.random.fold_in(arg_keys[5], 71), 0)
    ref_index = plant(jax.random.randint(arg_keys[1], (NELEM, NPTS), 0, REFS), jax.random.fold_in(arg_keys[1], 1), 0, REFS - 1).astype(jnp.int32)
    requests = draw_requests(jax.random.fold_in(arg_keys[5], 71), 0)
    source = draw_source(jax.random.fold_in(arg_keys[5], 71), 0)
    target_mean = jnp.clip(jnp.exp(jax.random.uniform(arg_keys[4], (TR,), jnp.float32, math.log(0.5), math.log(5.0))), 0.5, 5.0)
    return {"tracers": tracers, "ref_index": ref_index, "requests": requests, "source": source, "target_mean": target_mean}


def lagrange_table():
    side = math.isqrt(REFS)
    gll_nodes = [-1.0, -math.sqrt(0.2), math.sqrt(0.2), 1.0]
    points = -1.0 + 2.0 * jnp.arange(side, dtype=jnp.float32) / (side - 1)
    columns = []
    for which in range(4):
        basis = jnp.ones((side,), jnp.float32)
        for other in range(4):
            if other != which:
                basis = basis * (points - gll_nodes[other]) / (gll_nodes[which] - gll_nodes[other])
        columns.append(basis)
    one_dim = jnp.stack(columns, axis=1)
    return (one_dim[:, None, :, None] * one_dim[None, :, None, :]).reshape(side * side, 16)

def quadrature():
    edge = jnp.array([1.0 / 6.0, 5.0 / 6.0, 5.0 / 6.0, 1.0 / 6.0], jnp.float32)
    return (edge[:, None] * edge[None, :]).reshape(16)

def interpolate(source_rows, ref_index):
    elem_count, levels, width = source_rows.shape
    onehot = (ref_index[:, :, None] == jnp.arange(REFS, dtype=jnp.int32)[None, None, :]).astype(jnp.float32)
    matrix = jnp.einsum('epr,rn->epn', onehot, lagrange_table(), precision=lax.Precision.HIGHEST)
    values = source_rows.reshape(elem_count, levels * (width // 16), 16)
    result = jnp.einsum('epn,ecn->ecp', matrix, values, precision=lax.Precision.HIGHEST)
    lowest = lax.optimization_barrier(jnp.min(values, axis=2, keepdims=True))
    highest = lax.optimization_barrier(jnp.max(values, axis=2, keepdims=True))
    result = jnp.minimum(jnp.maximum(result, lowest), highest)
    return result.reshape(elem_count, levels, width)

def reference(tracers, ref_index, requests, source, target_mean):

    def block(device):
        first_row = device * ELEM_DEV
        left_dev = (device + N_ELEM - 1) % N_ELEM
        right_dev = (device + 1) % N_ELEM
        slots_here = lax.dynamic_slice_in_dim(source, first_row, ELEM_DEV, 0)
        refs_here = lax.dynamic_slice_in_dim(ref_index, first_row, ELEM_DEV, 0)
        wanted = requests[device]
        own_global = first_row + jnp.arange(ELEM_DEV, dtype=jnp.int32)
        left_global = left_dev * ELEM_DEV + jnp.maximum(wanted[0], 0)
        right_global = right_dev * ELEM_DEV + jnp.maximum(wanted[1], 0)
        slot_global = jnp.concatenate([own_global, left_global, right_global]).astype(jnp.int32)
        source_rows = tracers[slot_global[slots_here]]
        return interpolate(source_rows, refs_here)
    clipped = lax.map(block, jnp.arange(N_ELEM, dtype=jnp.int32))
    clipped = clipped.reshape(NELEM, NLEV, TR, NPTS)
    mass = jnp.einsum('eltn,n->t', clipped, quadrature(), precision=lax.Precision.HIGHEST)
    factor = target_mean * (4.0 * NELEM * NLEV) / mass
    return (clipped * factor[None, None, :, None]).reshape(NELEM, NLEV, TR * NPTS)
```

```python
import functools
import math

import jax
import jax.numpy as jnp
import numpy as np
from jax import lax
from jax.experimental import pallas as pl
from jax.experimental.pallas import tpu as pltpu
from jax.sharding import PartitionSpec as P

NPTS = 16
REFS = 64
LANES = 128
SUB = 8

VMEM = pltpu.VMEM
SMEM = pltpu.SMEM


def lagrange_1d():
    side = math.isqrt(REFS)
    nodes = [np.float32(v) for v in (-1.0, -math.sqrt(0.2), math.sqrt(0.2), 1.0)]
    points = (-1.0 + 2.0 * np.arange(side, dtype=np.float32) / np.float32(side - 1)).astype(np.float32)
    columns = []
    for which in range(4):
        basis = np.ones((side,), np.float32)
        for other in range(4):
            if other != which:
                basis = basis * (points - nodes[other]) / (nodes[which] - nodes[other])
        columns.append(basis)
    return np.stack(columns, axis=1)


SIDE = math.isqrt(REFS)
BASIS = lagrange_1d()
WEIGHT36 = [ci * cj for ci in (1, 5, 5, 1) for cj in (1, 5, 5, 1)]


def split3(x):
    a = x.astype(jnp.bfloat16)
    rest = x - a.astype(jnp.float32)
    b = rest.astype(jnp.bfloat16)
    c = (rest - b.astype(jnp.float32)).astype(jnp.bfloat16)
    return a, b, c


def onehot_dot(parts, onehot):
    return sum(jnp.dot(part, onehot, preferred_element_type=jnp.float32) for part in parts)


def mm_nt(a, b):
    return lax.dot_general(a, b, (((1,), (1,)), ((), ())), preferred_element_type=jnp.float32)


class Sizes:
    def __init__(self, elems, levels, width, slots):
        self.elems, self.levels, self.width, self.slots = elems, levels, width, slots
        self.tracers = width // NPTS
        self.per = LANES // elems
        self.nv = levels // self.per
        self.cols = levels * elems
        self.tiles = width // LANES
        self.tpt = LANES // NPTS
        self.halves = LANES // (levels * slots)
        self.part = width // self.halves


def plan_kernel(z, req_ref, ref_ref, src_ref, wown_ref, payl_ref, payr_ref, codes_ref, coef_ref):
    elems, slots, levels = z.elems, z.slots, z.levels
    src = src_ref[...]
    lane = lax.broadcasted_iota(jnp.int32, (1, LANES), 1)
    k_lane = lane % slots
    first = jnp.full((1, elems), -1, jnp.int32)
    second = first
    pat_l = jnp.zeros((1, LANES), jnp.int32)
    pat_r = pat_l
    for k in range(slots):
        left, right = req_ref[0, 0, k], req_ref[0, 1, k]
        first = jnp.where(src == elems + k, left, first)
        second = jnp.where(src == elems + slots + k, right, second)
        pat_l = jnp.where(k_lane == k, left, pat_l)
        pat_r = jnp.where(k_lane == k, right, pat_r)
    ref = ref_ref[...]
    row = lax.broadcasted_iota(jnp.int32, (REFS, elems), 0)
    counts = jnp.zeros((REFS, elems), jnp.float32)
    for p in range(NPTS):
        counts = counts + jnp.where(row == ref[p : p + 1, :], float(WEIGHT36[p]), 0.0)
    counts = counts.astype(jnp.bfloat16)
    srow = lax.broadcasted_iota(jnp.int32, (LANES, elems), 0) % elems

    def weights(which):
        return mm_nt(counts, (srow == which).astype(jnp.float32).astype(jnp.bfloat16))

    wown_ref[...] = weights(src)
    payl_ref[0:REFS, :] = weights(first)
    payl_ref[REFS : REFS + SUB, :] = jnp.broadcast_to(pat_l.astype(jnp.float32), (SUB, LANES))
    payr_ref[0:REFS, :] = weights(second)
    payr_ref[REFS : REFS + SUB, :] = jnp.broadcast_to(pat_r.astype(jnp.float32), (SUB, LANES))

    src2 = jnp.concatenate([src] * z.per, axis=1)
    sub_level = lane // elems
    for v in range(z.nv):
        level = sub_level + v * z.per
        at = slice(v * LANES, (v + 1) * LANES)
        codes_ref[0:1, at] = jnp.where(src2 < elems, level * elems + src2, -1)
        rel = src2 - elems
        side = jnp.where(rel >= slots, 1, 0)
        code = side * LANES + level * slots + (rel - side * slots)
        for h in range(z.halves):
            codes_ref[1 + h : 2 + h, at] = jnp.where(rel >= 0, code + h * levels * slots, -1)

    ref2 = jnp.concatenate([ref] * z.per, axis=1)
    one, two = ref2 // SIDE, ref2 % SIDE

    def basis(which):
        found = []
        for i in range(4):
            value = jnp.zeros(which.shape, jnp.float32)
            for a in range(SIDE):
                if BASIS[a, i] != 0.0:
                    value = jnp.where(which == a, float(BASIS[a, i]), value)
            found.append(value)
        return found

    la, lb = basis(one), basis(two)
    for i in range(4):
        for j in range(4):
            n = 4 * i + j
            coef_ref[n * NPTS : (n + 1) * NPTS, :] = la[i] * lb[j]


def line(x):
    out = [None] * SIDE
    out[0], out[SIDE - 1] = x[0], x[3]
    outer, inner = x[0] + x[3], x[1] + x[2]
    outer_odd, inner_odd = x[0] - x[3], x[1] - x[2]
    for a in range(1, SIDE // 2):
        c = [float(v) for v in BASIS[a]]
        even = (0.5 * (c[0] + c[3])) * outer + (0.5 * (c[1] + c[2])) * inner
        odd = (0.5 * (c[0] - c[3])) * outer_odd + (0.5 * (c[1] - c[2])) * inner_odd
        out[a], out[SIDE - 1 - a] = even + odd, even - odd
    return out


def tree(op, values):
    while len(values) > 1:
        values = [op(values[i], values[i + 1]) if i + 1 < len(values) else values[i] for i in range(0, len(values), 2)]
    return values[0]


def prep_kernel(z, x_ref, codes_ref, xt_ref, parts_ref, own_ref, sums_ref):
    step = z.tiles * z.levels
    for j in range(z.tiles):
        for v in range(z.nv):
            rows = []
            for q in range(z.per):
                level = v * z.per + q
                for e in range(0, z.elems, SUB):
                    rows.append(x_ref[pl.ds(e * step + j * z.levels + level, SUB, stride=step), :])
            block = jnp.concatenate(rows, axis=0)
            xt_ref[v, j * LANES : (j + 1) * LANES, :] = block.T
    a, b, c = split3(jnp.concatenate([xt_ref[v] for v in range(z.nv)], axis=1))
    parts_ref[0], parts_ref[1], parts_ref[2] = a, b, c
    row = lax.broadcasted_iota(jnp.int32, (z.cols, z.cols), 0)
    pick = (row == codes_ref[0:1, :]).astype(jnp.float32).astype(jnp.bfloat16)
    own_ref[...] = onehot_dot((a, b, c), pick)
    for j in range(z.tiles):
        both = [None] * REFS
        for v in range(z.nv):
            x = [xt_ref[v, pl.ds(j * LANES + n, z.tpt, stride=NPTS), :] for n in range(NPTS)]
            lowest, highest = tree(jnp.minimum, x), tree(jnp.maximum, x)
            lines = [line(x[4 * i : 4 * i + 4]) for i in range(4)]
            for b in range(SIDE):
                column = line([lines[i][b] for i in range(4)])
                for a in range(SIDE):
                    value = jnp.minimum(jnp.maximum(column[a], lowest), highest)
                    r = a * SIDE + b
                    both[r] = value if both[r] is None else both[r] + value
        for r in range(REFS):
            sums_ref[r * z.tracers + j * z.tpt : r * z.tracers + (j + 1) * z.tpt, :] = both[r]


def serve_kernel(z, wown_ref, inl_ref, inr_ref, sums_ref, parts_ref, mass_ref, tol_ref, tor_ref, weight_ref):
    weight_ref[...] = wown_ref[...] + inl_ref[0:REFS, :] + inr_ref[0:REFS, :]
    lane = lax.broadcasted_iota(jnp.int32, (1, LANES), 1)
    level = (lane // z.slots) % z.levels
    codes = []
    for ref in (inl_ref, inr_ref):
        wanted = ref[REFS : REFS + 1, :].astype(jnp.int32)
        codes.append(jnp.where(wanted >= 0, level * z.elems + wanted, -1))
    code = jnp.concatenate(codes, axis=1)
    row = lax.broadcasted_iota(jnp.int32, (z.cols, 2 * LANES), 0)
    pick = (row == code).astype(jnp.float32).astype(jnp.bfloat16)
    rows = onehot_dot((parts_ref[0], parts_ref[1], parts_ref[2]), pick)
    half = lane // (z.levels * z.slots)
    for ref, at in ((tor_ref, slice(0, LANES)), (tol_ref, slice(LANES, 2 * LANES))):
        value = rows[0 : z.part, at]
        for h in range(1, z.halves):
            value = jnp.where(half == h, rows[h * z.part : (h + 1) * z.part, at], value)
        ref[...] = value
    total = [None] * z.tiles
    for r in range(REFS):
        w = weight_ref[pl.ds(r, 1), :]
        for j in range(z.tiles):
            lo = r * z.tracers + j * z.tpt
            term = sums_ref[lo : lo + z.tpt, :] * w
            total[j] = term if total[j] is None else total[j] + term
    total = jnp.concatenate(total, axis=0)
    ones = jnp.ones((SUB, LANES), jnp.bfloat16)
    parts = split3(total)
    mass_ref[...] = sum(mm_nt(ones, part) for part in parts)[0:1, :]


def final_kernel(z, own_ref, froml_ref, fromr_ref, codes_ref, coef_ref, out_ref, got_ref, turn_ref):
    halo = jnp.concatenate([froml_ref[...], fromr_ref[...]], axis=1)
    parts = split3(halo)
    row = lax.broadcasted_iota(jnp.int32, (2 * LANES, z.cols), 0)
    for h in range(z.halves):
        pick = (row == codes_ref[1 + h : 2 + h, :]).astype(jnp.float32).astype(jnp.bfloat16)
        at = slice(h * z.part, (h + 1) * z.part)
        got = own_ref[at, :] + onehot_dot(parts, pick)
        for v in range(z.nv):
            got_ref[v, at, :] = got[:, v * LANES : (v + 1) * LANES]
    step = z.tiles * z.levels
    for j in range(z.tiles):
        xs, low, high = [], [], []
        for v in range(z.nv):
            x = [got_ref[v, pl.ds(j * LANES + n, z.tpt, stride=NPTS), :] for n in range(NPTS)]
            xs.append(x)
            low.append(tree(jnp.minimum, x))
            high.append(tree(jnp.maximum, x))
        for p in range(NPTS):
            coef = [coef_ref[pl.ds(n * NPTS + p, 1), :] for n in range(NPTS)]
            for v in range(z.nv):
                value = tree(jnp.add, [coef[n] * xs[v][n] for n in range(NPTS)])
                value = jnp.minimum(jnp.maximum(value, low[v]), high[v])
                turn_ref[v, pl.ds(p, z.tpt, stride=NPTS), :] = value
        for v in range(z.nv):
            block = turn_ref[v].T
            for q in range(z.per):
                level = v * z.per + q
                for e in range(0, z.elems, SUB):
                    piece = block[q * z.elems + e : q * z.elems + e + SUB, :]
                    out_ref[pl.ds(e * step + j * z.levels + level, SUB, stride=step), :] = piece


def call(kernel, z, name, outs, ins, args, scratch=(), flops=0, nbytes=0):
    return pl.pallas_call(
        functools.partial(kernel, z),
        out_shape=[jax.ShapeDtypeStruct(shape, dtype) for shape, dtype in outs],
        in_specs=[pl.BlockSpec(memory_space=space) for space in ins],
        out_specs=[pl.BlockSpec(memory_space=VMEM)] * len(outs),
        scratch_shapes=list(scratch),
        cost_estimate=pl.CostEstimate(flops=flops, bytes_accessed=nbytes, transcendentals=0),
        name=name,
    )(*args)


def per_device(tracers, ref_index, requests, source, target_mean):
    elems, levels, width = tracers.shape
    z = Sizes(elems, levels, width, requests.shape[2])
    assert z.per * elems == LANES and z.nv * z.per == levels and z.tiles * LANES == width
    assert z.halves * levels * z.slots == LANES and z.part * z.halves == width
    f32, bf16, i32 = jnp.float32, jnp.bfloat16, jnp.int32
    flat = tracers.reshape(elems, levels, z.tiles, LANES).transpose(0, 2, 1, 3).reshape(-1, LANES)

    wown, payl, payr, codes, coef = call(
        plan_kernel, z, "plan",
        [((REFS, LANES), f32), ((REFS + SUB, LANES), f32), ((REFS + SUB, LANES), f32), ((SUB, z.cols), i32),
         ((NPTS * NPTS, LANES), f32)],
        (SMEM, VMEM, VMEM), (requests, ref_index.T, source.reshape(1, elems)), flops=10**6, nbytes=10**5,
    )
    count = lax.axis_size("elem")
    to_right = [(i, (i + 1) % count) for i in range(count)]
    to_left = [((i + 1) % count, i) for i in range(count)]
    inl = lax.ppermute(payl, "elem", to_left)
    inr = lax.ppermute(payr, "elem", to_right)
    _, parts, own, sums = call(
        prep_kernel, z, "prep",
        [((z.nv, width, LANES), f32), ((3, width, z.cols), bf16), ((width, z.cols), f32), ((REFS * z.tracers, LANES), f32)],
        (VMEM, VMEM), (flat, codes), flops=10**8, nbytes=4 * 10**6,
    )
    mass, tol, tor = call(
        serve_kernel, z, "serve",
        [((1, z.tracers), f32), ((z.part, LANES), f32), ((z.part, LANES), f32)],
        (VMEM,) * 5, (wown, inl, inr, sums, parts), [VMEM((REFS, LANES), f32)], flops=10**7, nbytes=3 * 10**6,
    )
    froml = lax.ppermute(tor, "elem", to_right)
    fromr = lax.ppermute(tol, "elem", to_left)
    axes = ("elem", "lev")
    members = lax.axis_size(axes)
    spread = jnp.broadcast_to(mass[None], (members, 1, z.tracers))
    every = lax.all_to_all(spread, axes, 0, 0)
    (shaped,) = call(
        final_kernel, z, "final",
        [((elems * levels * z.tiles, LANES), f32)],
        (VMEM,) * 5, (own, froml, fromr, codes, coef),
        [VMEM((z.nv, width, LANES), f32), VMEM((z.nv, LANES, LANES), f32)], flops=10**8, nbytes=3 * 10**6,
    )
    shaped = shaped.reshape(elems, z.tiles, levels, LANES).transpose(0, 2, 1, 3).reshape(elems, levels, width)
    global_mass = every.sum(axis=(0, 1))
    whole_weight = 36.0 * 4.0 * elems * count * levels * lax.axis_size("lev")
    factor = target_mean * whole_weight / global_mass
    return shaped * jnp.repeat(factor, NPTS)[None, None, :]


def solution(mesh):
    placed = (P("elem", "lev", None), P("elem", None), P("elem", None, None), P("elem"), P())
    return jax.shard_map(
        per_device, mesh=mesh, in_specs=placed, out_specs=P("elem", "lev", None), check_vma=False
    )
```

```python
import functools
import math

import jax
import jax.numpy as jnp
import numpy as np
from jax import lax
from jax.experimental import pallas as pl
from jax.experimental.pallas import tpu as pltpu
from jax.sharding import PartitionSpec as P


NPTS = 16
REFS = 64
LANES = 128
SUB = 8

VMEM = pltpu.VMEM
SMEM = pltpu.SMEM


def lagrange_1d():
    side = math.isqrt(REFS)
    nodes = [np.float32(v) for v in (-1.0, -math.sqrt(0.2), math.sqrt(0.2), 1.0)]
    points = (-1.0 + 2.0 * np.arange(side, dtype=np.float32) / np.float32(side - 1)).astype(np.float32)
    columns = []
    for which in range(4):
        basis = np.ones((side,), np.float32)
        for other in range(4):
            if other != which:
                basis = basis * (points - nodes[other]) / (nodes[which] - nodes[other])
        columns.append(basis)
    return np.stack(columns, axis=1)


SIDE = math.isqrt(REFS)
BASIS = lagrange_1d()
WEIGHT36 = [ci * cj for ci in (1, 5, 5, 1) for cj in (1, 5, 5, 1)]


def split3(x):
    a = x.astype(jnp.bfloat16)
    rest = x - a.astype(jnp.float32)
    b = rest.astype(jnp.bfloat16)
    c = (rest - b.astype(jnp.float32)).astype(jnp.bfloat16)
    return a, b, c


def onehot_dot(parts, onehot):
    return sum(jnp.dot(part, onehot, preferred_element_type=jnp.float32) for part in parts)


def mm_nt(a, b):
    return lax.dot_general(a, b, (((1,), (1,)), ((), ())), preferred_element_type=jnp.float32)


class Sizes:
    def __init__(self, elems, levels, width, slots):
        self.elems, self.levels, self.width, self.slots = elems, levels, width, slots
        self.tracers = width // NPTS
        self.per = LANES // elems
        self.nv = levels // self.per
        self.cols = levels * elems
        self.tiles = width // LANES
        self.tpt = LANES // NPTS
        self.halves = LANES // (levels * slots)
        self.part = width // self.halves


def plan_kernel(
    z, x_hbm, req_hbm, ref_hbm, src_hbm, wown_ref, payl_ref, payr_ref, raw_ref, ref_ref, src_ref, req_ref, sem, xsem
):
    elems, slots = z.elems, z.slots
    small = [
        pltpu.make_async_copy(src, dst, sem.at[i])
        for i, (src, dst) in enumerate(((req_hbm, req_ref), (ref_hbm, ref_ref), (src_hbm, src_ref)))
    ]
    large = [
        pltpu.make_async_copy(
            x_hbm.at[:, :, pl.ds(j * LANES, LANES)], raw_ref.at[j].reshape(elems, z.levels, LANES), xsem.at[j]
        )
        for j in range(z.tiles)
    ]
    for copy in small + large:
        copy.start()
    for copy in small:
        copy.wait()
    src = src_ref[...]
    lane = lax.broadcasted_iota(jnp.int32, (1, LANES), 1)
    k_lane = lane % slots
    first = jnp.full((1, elems), -1, jnp.int32)
    second = first
    pat_l = jnp.zeros((1, LANES), jnp.int32)
    pat_r = pat_l
    for k in range(slots):
        left, right = req_ref[0, 0, k], req_ref[0, 1, k]
        first = jnp.where(src == elems + k, left, first)
        second = jnp.where(src == elems + slots + k, right, second)
        pat_l = jnp.where(k_lane == k, left, pat_l)
        pat_r = jnp.where(k_lane == k, right, pat_r)
    ref = ref_ref[...]
    row = lax.broadcasted_iota(jnp.int32, (REFS, elems), 0)
    counts = jnp.zeros((REFS, elems), jnp.float32)
    for p in range(NPTS):
        counts = counts + jnp.where(row == ref[p : p + 1, :], float(WEIGHT36[p]), 0.0)
    counts = counts.astype(jnp.bfloat16)
    srow = lax.broadcasted_iota(jnp.int32, (LANES, elems), 0) % elems

    def weights(which):
        return mm_nt(counts, (srow == which).astype(jnp.float32).astype(jnp.bfloat16))

    wown_ref[...] = weights(src)
    payl_ref[0:REFS, :] = weights(first)
    payl_ref[REFS : REFS + SUB, :] = jnp.broadcast_to(pat_l.astype(jnp.float32), (SUB, LANES))
    payr_ref[0:REFS, :] = weights(second)
    payr_ref[REFS : REFS + SUB, :] = jnp.broadcast_to(pat_r.astype(jnp.float32), (SUB, LANES))
    for copy in large:
        copy.wait()


def tables(z, src, ref, codes_ref, coef_ref):
    elems, slots, levels = z.elems, z.slots, z.levels
    lane = lax.broadcasted_iota(jnp.int32, (1, LANES), 1)
    src2 = jnp.concatenate([src] * z.per, axis=1)
    sub_level = lane // elems
    for v in range(z.nv):
        level = sub_level + v * z.per
        at = slice(v * LANES, (v + 1) * LANES)
        codes_ref[0:1, at] = jnp.where(src2 < elems, level * elems + src2, -1)
        rel = src2 - elems
        side = jnp.where(rel >= slots, 1, 0)
        code = side * LANES + level * slots + (rel - side * slots)
        for h in range(z.halves):
            codes_ref[1 + h : 2 + h, at] = jnp.where(rel >= 0, code + h * levels * slots, -1)

    ref2 = jnp.concatenate([ref] * z.per, axis=1)
    one, two = ref2 // SIDE, ref2 % SIDE

    def basis(which):
        found = []
        for i in range(4):
            value = jnp.zeros(which.shape, jnp.float32)
            for a in range(SIDE):
                if BASIS[a, i] != 0.0:
                    value = jnp.where(which == a, float(BASIS[a, i]), value)
            found.append(value)
        return found

    la, lb = basis(one), basis(two)
    for i in range(4):
        for j in range(4):
            n = 4 * i + j
            coef_ref[n * NPTS : (n + 1) * NPTS, :] = la[i] * lb[j]


def line(x):
    out = [None] * SIDE
    out[0], out[SIDE - 1] = x[0], x[3]
    outer, inner = x[0] + x[3], x[1] + x[2]
    outer_odd, inner_odd = x[0] - x[3], x[1] - x[2]
    for a in range(1, SIDE // 2):
        c = [float(v) for v in BASIS[a]]
        even = (0.5 * (c[0] + c[3])) * outer + (0.5 * (c[1] + c[2])) * inner
        odd = (0.5 * (c[0] - c[3])) * outer_odd + (0.5 * (c[1] - c[2])) * inner_odd
        out[a], out[SIDE - 1 - a] = even + odd, even - odd
    return out


def tree(op, values):
    while len(values) > 1:
        values = [op(values[i], values[i + 1]) if i + 1 < len(values) else values[i] for i in range(0, len(values), 2)]
    return values[0]


def prep_kernel(z, raw_ref, ref_ref, src_ref, parts_ref, own_ref, sums_ref, codes_ref, coef_ref, xt_ref):
    tables(z, src_ref[...], ref_ref[...], codes_ref, coef_ref)
    for j in range(z.tiles):
        for v in range(z.nv):
            rows = []
            for q in range(z.per):
                level = v * z.per + q
                for e in range(0, z.elems, SUB):
                    rows.append(raw_ref[j, pl.ds(e * z.levels + level, SUB, stride=z.levels), :])
            block = jnp.concatenate(rows, axis=0)
            xt_ref[v, j * LANES : (j + 1) * LANES, :] = block.T
    a, b, c = split3(jnp.concatenate([xt_ref[v] for v in range(z.nv)], axis=1))
    parts_ref[0], parts_ref[1], parts_ref[2] = a, b, c
    row = lax.broadcasted_iota(jnp.int32, (z.cols, z.cols), 0)
    pick = (row == codes_ref[0:1, :]).astype(jnp.float32).astype(jnp.bfloat16)
    own_ref[...] = onehot_dot((a, b, c), pick)
    for j in range(z.tiles):
        both = [None] * REFS
        for v in range(z.nv):
            x = [xt_ref[v, pl.ds(j * LANES + n, z.tpt, stride=NPTS), :] for n in range(NPTS)]
            lowest, highest = tree(jnp.minimum, x), tree(jnp.maximum, x)
            lines = [line(x[4 * i : 4 * i + 4]) for i in range(4)]
            for b in range(SIDE):
                column = line([lines[i][b] for i in range(4)])
                for a in range(SIDE):
                    value = jnp.minimum(jnp.maximum(column[a], lowest), highest)
                    r = a * SIDE + b
                    both[r] = value if both[r] is None else both[r] + value
        for r in range(REFS):
            sums_ref[r * z.tracers + j * z.tpt : r * z.tracers + (j + 1) * z.tpt, :] = both[r]


def serve_kernel(z, wown_ref, inl_ref, inr_ref, sums_ref, parts_ref, mass_ref, tol_ref, tor_ref, weight_ref):
    weight_ref[...] = wown_ref[...] + inl_ref[0:REFS, :] + inr_ref[0:REFS, :]
    lane = lax.broadcasted_iota(jnp.int32, (1, LANES), 1)
    level = (lane // z.slots) % z.levels
    codes = []
    for ref in (inl_ref, inr_ref):
        wanted = ref[REFS : REFS + 1, :].astype(jnp.int32)
        codes.append(jnp.where(wanted >= 0, level * z.elems + wanted, -1))
    code = jnp.concatenate(codes, axis=1)
    row = lax.broadcasted_iota(jnp.int32, (z.cols, 2 * LANES), 0)
    pick = (row == code).astype(jnp.float32).astype(jnp.bfloat16)
    rows = onehot_dot((parts_ref[0], parts_ref[1], parts_ref[2]), pick)
    half = lane // (z.levels * z.slots)
    for ref, at in ((tor_ref, slice(0, LANES)), (tol_ref, slice(LANES, 2 * LANES))):
        value = rows[0 : z.part, at]
        for h in range(1, z.halves):
            value = jnp.where(half == h, rows[h * z.part : (h + 1) * z.part, at], value)
        ref[...] = value
    total = [None] * z.tiles
    for r in range(REFS):
        w = weight_ref[pl.ds(r, 1), :]
        for j in range(z.tiles):
            lo = r * z.tracers + j * z.tpt
            term = sums_ref[lo : lo + z.tpt, :] * w
            total[j] = term if total[j] is None else total[j] + term
    total = jnp.concatenate(total, axis=0)
    ones = jnp.ones((SUB, LANES), jnp.bfloat16)
    parts = split3(total)
    mass_ref[...] = sum(mm_nt(ones, part) for part in parts)[0:1, :]


def final_kernel(z, own_ref, froml_ref, fromr_ref, codes_ref, coef_ref, out_ref, got_ref, turn_ref, flat_ref, sem):
    halo = jnp.concatenate([froml_ref[...], fromr_ref[...]], axis=1)
    parts = split3(halo)
    row = lax.broadcasted_iota(jnp.int32, (2 * LANES, z.cols), 0)
    for h in range(z.halves):
        pick = (row == codes_ref[1 + h : 2 + h, :]).astype(jnp.float32).astype(jnp.bfloat16)
        at = slice(h * z.part, (h + 1) * z.part)
        got = own_ref[at, :] + onehot_dot(parts, pick)
        for v in range(z.nv):
            got_ref[v, at, :] = got[:, v * LANES : (v + 1) * LANES]
    copies = []
    for j in range(z.tiles):
        xs, low, high = [], [], []
        for v in range(z.nv):
            x = [got_ref[v, pl.ds(j * LANES + n, z.tpt, stride=NPTS), :] for n in range(NPTS)]
            xs.append(x)
            low.append(tree(jnp.minimum, x))
            high.append(tree(jnp.maximum, x))
        for p in range(NPTS):
            coef = [coef_ref[pl.ds(n * NPTS + p, 1), :] for n in range(NPTS)]
            for v in range(z.nv):
                value = tree(jnp.add, [coef[n] * xs[v][n] for n in range(NPTS)])
                value = jnp.minimum(jnp.maximum(value, low[v]), high[v])
                turn_ref[v, pl.ds(p, z.tpt, stride=NPTS), :] = value
        for v in range(z.nv):
            block = turn_ref[v].T
            for q in range(z.per):
                level = v * z.per + q
                for e in range(0, z.elems, SUB):
                    piece = block[q * z.elems + e : q * z.elems + e + SUB, :]
                    flat_ref[j, pl.ds(e * z.levels + level, SUB, stride=z.levels), :] = piece
        copies.append(
            pltpu.make_async_copy(
                flat_ref.at[j].reshape(z.elems, z.levels, LANES), out_ref.at[:, :, pl.ds(j * LANES, LANES)], sem.at[j]
            )
        )
        copies[-1].start()
    for copy in copies:
        copy.wait()


def in_hbm(x):
    return pltpu.with_memory_space_constraint(x, pltpu.HBM)


def call(kernel, z, outs, ins, args, scratch=(), flops=0, nbytes=0, limit=16):
    return pl.pallas_call(
        functools.partial(kernel, z),
        out_shape=[jax.ShapeDtypeStruct(shape, dtype) for shape, dtype in outs],
        in_specs=[pl.BlockSpec(memory_space=space) for space in ins],
        out_specs=[pl.BlockSpec(memory_space=VMEM)] * len(outs),
        scratch_shapes=list(scratch),
        cost_estimate=pl.CostEstimate(flops=flops, bytes_accessed=nbytes, transcendentals=0),
        compiler_params=pltpu.CompilerParams(vmem_limit_bytes=limit << 20),
    )(*args)


def per_device(tracers, ref_index, requests, source, target_mean):
    elems, levels, width = tracers.shape
    z = Sizes(elems, levels, width, requests.shape[2])
    assert z.per * elems == LANES and z.nv * z.per == levels and z.tiles * LANES == width
    assert z.halves * levels * z.slots == LANES and z.part * z.halves == width
    f32, bf16, i32 = jnp.float32, jnp.bfloat16, jnp.int32
    flat = ((z.tiles, elems * levels, LANES), f32)
    wown, payl, payr, raw, refs, own_source = call(
        plan_kernel, z,
        [((REFS, LANES), f32), ((REFS + SUB, LANES), f32), ((REFS + SUB, LANES), f32), flat,
         ((NPTS, elems), i32), ((1, elems), i32)],
        (pltpu.HBM,) * 4, [in_hbm(a) for a in (tracers, requests, ref_index.T, source.reshape(1, elems))],
        [SMEM(requests.shape, i32), pltpu.SemaphoreType.DMA((3,)), pltpu.SemaphoreType.DMA((z.tiles,))],
        flops=10**6, nbytes=10**5,
    )
    count = lax.axis_size("elem")
    to_right = [(i, (i + 1) % count) for i in range(count)]
    to_left = [((i + 1) % count, i) for i in range(count)]
    inl = lax.ppermute(payl, "elem", to_left)
    inr = lax.ppermute(payr, "elem", to_right)
    parts, own, sums, codes, coef = call(
        prep_kernel, z,
        [((3, width, z.cols), bf16), ((width, z.cols), f32), ((REFS * z.tracers, LANES), f32), ((SUB, z.cols), i32),
         ((NPTS * NPTS, LANES), f32)],
        (VMEM,) * 3, (raw, refs, own_source), [VMEM((z.nv, width, LANES), f32)], flops=10**8, nbytes=4 * 10**6,
    )
    mass, tol, tor = call(
        serve_kernel, z,
        [((1, z.tracers), f32), ((z.part, LANES), f32), ((z.part, LANES), f32)],
        (VMEM,) * 5, (wown, inl, inr, sums, parts), [VMEM((REFS, LANES), f32)], flops=10**7, nbytes=3 * 10**6,
    )
    froml = lax.ppermute(tor, "elem", to_right)
    fromr = lax.ppermute(tol, "elem", to_left)
    axes = ("elem", "lev")
    members = lax.axis_size(axes)
    spread = jnp.broadcast_to(mass[None], (members, 1, z.tracers))
    every = lax.all_to_all(spread, axes, 0, 0)
    (shaped,) = call(
        final_kernel, z,
        [((elems, levels, width), f32)],
        (VMEM,) * 5, (own, froml, fromr, codes, coef),
        [VMEM((z.nv, width, LANES), f32), VMEM((z.nv, LANES, LANES), f32), VMEM(*flat), pltpu.SemaphoreType.DMA((z.tiles,))],
        flops=10**8, nbytes=3 * 10**6,
    )
    global_mass = every.sum(axis=(0, 1))
    whole_weight = 36.0 * 4.0 * elems * count * levels * lax.axis_size("lev")
    factor = target_mean * whole_weight / global_mass
    return shaped * jnp.repeat(factor, NPTS)[None, None, :]


def solution(mesh):
    placed = (P("elem", "lev", None), P("elem", None), P("elem", None, None), P("elem"), P())

    return jax.shard_map(per_device, mesh=mesh, in_specs=placed, out_specs=P("elem", "lev", None), check_vma=False)
```

```python
import functools
import math

import jax
import jax.numpy as jnp
import numpy as np
from jax import lax
from jax.experimental import pallas as pl
from jax.experimental.pallas import tpu as pltpu
from jax.sharding import PartitionSpec as P


NPTS = 16
REFS = 64
LANES = 128
SUB = 8

VMEM = pltpu.VMEM
SMEM = pltpu.SMEM


def lagrange_1d():
    side = math.isqrt(REFS)
    nodes = [np.float32(v) for v in (-1.0, -math.sqrt(0.2), math.sqrt(0.2), 1.0)]
    points = (-1.0 + 2.0 * np.arange(side, dtype=np.float32) / np.float32(side - 1)).astype(np.float32)
    columns = []
    for which in range(4):
        basis = np.ones((side,), np.float32)
        for other in range(4):
            if other != which:
                basis = basis * (points - nodes[other]) / (nodes[which] - nodes[other])
        columns.append(basis)
    return np.stack(columns, axis=1)


SIDE = math.isqrt(REFS)
BASIS = lagrange_1d()
WEIGHT36 = [ci * cj for ci in (1, 5, 5, 1) for cj in (1, 5, 5, 1)]


def split3(x):
    a = x.astype(jnp.bfloat16)
    rest = x - a.astype(jnp.float32)
    b = rest.astype(jnp.bfloat16)
    c = (rest - b.astype(jnp.float32)).astype(jnp.bfloat16)
    return a, b, c


def onehot_dot(parts, onehot):
    return sum(jnp.dot(part, onehot, preferred_element_type=jnp.float32) for part in parts)


def mm_nt(a, b):
    return lax.dot_general(a, b, (((1,), (1,)), ((), ())), preferred_element_type=jnp.float32)


class Sizes:
    def __init__(self, elems, levels, width, slots):
        self.elems, self.levels, self.width, self.slots = elems, levels, width, slots
        self.tracers = width // NPTS
        self.per = LANES // elems
        self.nv = levels // self.per
        self.cols = levels * elems
        self.tiles = width // LANES
        self.tpt = LANES // NPTS
        self.halves = LANES // (levels * slots)
        self.part = width // self.halves


def plan_kernel(
    z, x_hbm, req_hbm, ref_hbm, src_hbm, wown_ref, far_ref, near_ref, raw_ref, ref_ref, src_ref, req_ref, sem, xsem
):
    elems, slots = z.elems, z.slots
    small = [
        pltpu.make_async_copy(src, dst, sem.at[i])
        for i, (src, dst) in enumerate(((req_hbm, req_ref), (ref_hbm, ref_ref), (src_hbm, src_ref)))
    ]
    large = [
        pltpu.make_async_copy(
            x_hbm.at[:, :, pl.ds(j * LANES, LANES)], raw_ref.at[j].reshape(elems, z.levels, LANES), xsem.at[j]
        )
        for j in range(z.tiles)
    ]
    for copy in small + large:
        copy.start()
    for copy in small:
        copy.wait()
    src = src_ref[...]
    lane = lax.broadcasted_iota(jnp.int32, (1, LANES), 1)
    k_lane = lane % slots
    odd = lax.rem(lax.axis_index("elem"), 2)
    far_base, near_base = elems + odd * slots, elems + (1 - odd) * slots
    far = jnp.full((1, elems), -1, jnp.int32)
    near = far
    pat_far = jnp.zeros((1, LANES), jnp.int32)
    pat_near = pat_far
    for k in range(slots):
        far_k, near_k = req_ref[0, odd, k], req_ref[0, 1 - odd, k]
        far = jnp.where(src == far_base + k, far_k, far)
        near = jnp.where(src == near_base + k, near_k, near)
        pat_far = jnp.where(k_lane == k, far_k, pat_far)
        pat_near = jnp.where(k_lane == k, near_k, pat_near)
    ref = ref_ref[...]
    row = lax.broadcasted_iota(jnp.int32, (REFS, elems), 0)
    counts = jnp.zeros((REFS, elems), jnp.float32)
    for p in range(NPTS):
        counts = counts + jnp.where(row == ref[p : p + 1, :], float(WEIGHT36[p]), 0.0)
    counts = counts.astype(jnp.bfloat16)
    srow = lax.broadcasted_iota(jnp.int32, (LANES, elems), 0) % elems

    def weights(which):
        return mm_nt(counts, (srow == which).astype(jnp.float32).astype(jnp.bfloat16))

    wown_ref[...] = weights(src)
    far_ref[0:REFS, :] = weights(far)
    far_ref[REFS : REFS + SUB, :] = jnp.broadcast_to(pat_far.astype(jnp.float32), (SUB, LANES))
    near_ref[0:REFS, :] = weights(near)
    near_ref[REFS : REFS + SUB, :] = jnp.broadcast_to(pat_near.astype(jnp.float32), (SUB, LANES))
    for copy in large:
        copy.wait()


def tables(z, src, ref, codes_ref, coef_ref):
    elems, slots, levels = z.elems, z.slots, z.levels
    odd = lax.rem(lax.axis_index("elem"), 2)
    lane = lax.broadcasted_iota(jnp.int32, (1, LANES), 1)
    src2 = jnp.concatenate([src] * z.per, axis=1)
    sub_level = lane // elems
    for v in range(z.nv):
        level = sub_level + v * z.per
        at = slice(v * LANES, (v + 1) * LANES)
        codes_ref[0:1, at] = jnp.where(src2 < elems, level * elems + src2, -1)
        rel = src2 - elems
        side = jnp.where(rel >= slots, 1, 0)
        code = jnp.where(side == odd, 0, LANES) + level * slots + (rel - side * slots)
        for h in range(z.halves):
            codes_ref[1 + h : 2 + h, at] = jnp.where(rel >= 0, code + h * levels * slots, -1)

    ref2 = jnp.concatenate([ref] * z.per, axis=1)
    one, two = ref2 // SIDE, ref2 % SIDE

    def basis(which):
        found = []
        for i in range(4):
            value = jnp.zeros(which.shape, jnp.float32)
            for a in range(SIDE):
                if BASIS[a, i] != 0.0:
                    value = jnp.where(which == a, float(BASIS[a, i]), value)
            found.append(value)
        return found

    la, lb = basis(one), basis(two)
    for i in range(4):
        for j in range(4):
            n = 4 * i + j
            coef_ref[n * NPTS : (n + 1) * NPTS, :] = la[i] * lb[j]


def line(x):
    out = [None] * SIDE
    out[0], out[SIDE - 1] = x[0], x[3]
    outer, inner = x[0] + x[3], x[1] + x[2]
    outer_odd, inner_odd = x[0] - x[3], x[1] - x[2]
    for a in range(1, SIDE // 2):
        c = [float(v) for v in BASIS[a]]
        even = (0.5 * (c[0] + c[3])) * outer + (0.5 * (c[1] + c[2])) * inner
        odd = (0.5 * (c[0] - c[3])) * outer_odd + (0.5 * (c[1] - c[2])) * inner_odd
        out[a], out[SIDE - 1 - a] = even + odd, even - odd
    return out


def tree(op, values):
    while len(values) > 1:
        values = [op(values[i], values[i + 1]) if i + 1 < len(values) else values[i] for i in range(0, len(values), 2)]
    return values[0]


def prep_kernel(z, raw_ref, ref_ref, src_ref, parts_ref, own_ref, sums_ref, codes_ref, coef_ref, xt_ref):
    tables(z, src_ref[...], ref_ref[...], codes_ref, coef_ref)
    for j in range(z.tiles):
        for v in range(z.nv):
            rows = []
            for q in range(z.per):
                level = v * z.per + q
                for e in range(0, z.elems, SUB):
                    rows.append(raw_ref[j, pl.ds(e * z.levels + level, SUB, stride=z.levels), :])
            block = jnp.concatenate(rows, axis=0)
            xt_ref[v, j * LANES : (j + 1) * LANES, :] = block.T
    a, b, c = split3(jnp.concatenate([xt_ref[v] for v in range(z.nv)], axis=1))
    parts_ref[0], parts_ref[1], parts_ref[2] = a, b, c
    row = lax.broadcasted_iota(jnp.int32, (z.cols, z.cols), 0)
    pick = (row == codes_ref[0:1, :]).astype(jnp.float32).astype(jnp.bfloat16)
    own_ref[...] = onehot_dot((a, b, c), pick)
    for j in range(z.tiles):
        both = [None] * REFS
        for v in range(z.nv):
            x = [xt_ref[v, pl.ds(j * LANES + n, z.tpt, stride=NPTS), :] for n in range(NPTS)]
            lowest, highest = tree(jnp.minimum, x), tree(jnp.maximum, x)
            lines = [line(x[4 * i : 4 * i + 4]) for i in range(4)]
            for b in range(SIDE):
                column = line([lines[i][b] for i in range(4)])
                for a in range(SIDE):
                    value = jnp.minimum(jnp.maximum(column[a], lowest), highest)
                    r = a * SIDE + b
                    both[r] = value if both[r] is None else both[r] + value
        for r in range(REFS):
            sums_ref[r * z.tracers + j * z.tpt : r * z.tracers + (j + 1) * z.tpt, :] = both[r]


def serve_kernel(z, wown_ref, infar_ref, innear_ref, sums_ref, parts_ref, mass_ref, tofar_ref, tonear_ref, weight_ref):
    weight_ref[...] = wown_ref[...] + infar_ref[0:REFS, :] + innear_ref[0:REFS, :]
    lane = lax.broadcasted_iota(jnp.int32, (1, LANES), 1)
    level = (lane // z.slots) % z.levels
    codes = []
    for ref in (infar_ref, innear_ref):
        wanted = ref[REFS : REFS + 1, :].astype(jnp.int32)
        codes.append(jnp.where(wanted >= 0, level * z.elems + wanted, -1))
    code = jnp.concatenate(codes, axis=1)
    row = lax.broadcasted_iota(jnp.int32, (z.cols, 2 * LANES), 0)
    pick = (row == code).astype(jnp.float32).astype(jnp.bfloat16)
    rows = onehot_dot((parts_ref[0], parts_ref[1], parts_ref[2]), pick)
    half = lane // (z.levels * z.slots)
    for ref, at in ((tofar_ref, slice(0, LANES)), (tonear_ref, slice(LANES, 2 * LANES))):
        value = rows[0 : z.part, at]
        for h in range(1, z.halves):
            value = jnp.where(half == h, rows[h * z.part : (h + 1) * z.part, at], value)
        ref[...] = value
    total = [None] * z.tiles
    for r in range(REFS):
        w = weight_ref[pl.ds(r, 1), :]
        for j in range(z.tiles):
            lo = r * z.tracers + j * z.tpt
            term = sums_ref[lo : lo + z.tpt, :] * w
            total[j] = term if total[j] is None else total[j] + term
    total = jnp.concatenate(total, axis=0)
    ones = jnp.ones((SUB, LANES), jnp.bfloat16)
    parts = split3(total)
    mass = sum(mm_nt(ones, part) for part in parts)[0:1, :]
    mass_ref[...] = jnp.broadcast_to(mass[None], mass_ref.shape)


def final_kernel(z, own_ref, far_ref, near_ref, codes_ref, coef_ref, out_ref, got_ref, turn_ref, flat_ref, sem):
    halo = jnp.concatenate([far_ref[...], near_ref[...]], axis=1)
    parts = split3(halo)
    row = lax.broadcasted_iota(jnp.int32, (2 * LANES, z.cols), 0)
    for h in range(z.halves):
        pick = (row == codes_ref[1 + h : 2 + h, :]).astype(jnp.float32).astype(jnp.bfloat16)
        at = slice(h * z.part, (h + 1) * z.part)
        got = own_ref[at, :] + onehot_dot(parts, pick)
        for v in range(z.nv):
            got_ref[v, at, :] = got[:, v * LANES : (v + 1) * LANES]
    copies = []
    for j in range(z.tiles):
        xs, low, high = [], [], []
        for v in range(z.nv):
            x = [got_ref[v, pl.ds(j * LANES + n, z.tpt, stride=NPTS), :] for n in range(NPTS)]
            xs.append(x)
            low.append(tree(jnp.minimum, x))
            high.append(tree(jnp.maximum, x))
        for p in range(NPTS):
            coef = [coef_ref[pl.ds(n * NPTS + p, 1), :] for n in range(NPTS)]
            for v in range(z.nv):
                value = tree(jnp.add, [coef[n] * xs[v][n] for n in range(NPTS)])
                value = jnp.minimum(jnp.maximum(value, low[v]), high[v])
                turn_ref[v, pl.ds(p, z.tpt, stride=NPTS), :] = value
        for v in range(z.nv):
            block = turn_ref[v].T
            for q in range(z.per):
                level = v * z.per + q
                for e in range(0, z.elems, SUB):
                    piece = block[q * z.elems + e : q * z.elems + e + SUB, :]
                    flat_ref[j, pl.ds(e * z.levels + level, SUB, stride=z.levels), :] = piece
        copies.append(
            pltpu.make_async_copy(
                flat_ref.at[j].reshape(z.elems, z.levels, LANES), out_ref.at[:, :, pl.ds(j * LANES, LANES)], sem.at[j]
            )
        )
        copies[-1].start()
    for copy in copies:
        copy.wait()


def in_hbm(x):
    return pltpu.with_memory_space_constraint(x, pltpu.HBM)


def call(kernel, z, outs, ins, args, scratch=(), flops=0, nbytes=0, limit=16):
    return pl.pallas_call(
        functools.partial(kernel, z),
        out_shape=[jax.ShapeDtypeStruct(shape, dtype) for shape, dtype in outs],
        in_specs=[pl.BlockSpec(memory_space=space) for space in ins],
        out_specs=[pl.BlockSpec(memory_space=VMEM)] * len(outs),
        scratch_shapes=list(scratch),
        cost_estimate=pl.CostEstimate(flops=flops, bytes_accessed=nbytes, transcendentals=0),
        compiler_params=pltpu.CompilerParams(vmem_limit_bytes=limit << 20),
    )(*args)


def per_device(tracers, ref_index, requests, source, target_mean):
    elems, levels, width = tracers.shape
    z = Sizes(elems, levels, width, requests.shape[2])
    assert z.per * elems == LANES and z.nv * z.per == levels and z.tiles * LANES == width
    assert z.halves * levels * z.slots == LANES and z.part * z.halves == width
    f32, bf16, i32 = jnp.float32, jnp.bfloat16, jnp.int32
    flat = ((z.tiles, elems * levels, LANES), f32)
    wown, ask_far, ask_near, raw, refs, own_source = call(
        plan_kernel, z,
        [((REFS, LANES), f32), ((REFS + SUB, LANES), f32), ((REFS + SUB, LANES), f32), flat,
         ((NPTS, elems), i32), ((1, elems), i32)],
        (pltpu.HBM,) * 4, [in_hbm(a) for a in (tracers, requests, ref_index.T, source.reshape(1, elems))],
        [SMEM(requests.shape, i32), pltpu.SemaphoreType.DMA((3,)), pltpu.SemaphoreType.DMA((z.tiles,))],
        flops=10**6, nbytes=10**5,
    )
    count = lax.axis_size("elem")
    assert count % 2 == 0
    far = [(i, (i - 1 if i % 2 == 0 else i + 1) % count) for i in range(count)]
    near = [(i, i + 1 if i % 2 == 0 else i - 1) for i in range(count)]
    in_far = lax.ppermute(ask_far, "elem", far)
    in_near = lax.ppermute(ask_near, "elem", near)
    parts, own, sums, codes, coef = call(
        prep_kernel, z,
        [((3, width, z.cols), bf16), ((width, z.cols), f32), ((REFS * z.tracers, LANES), f32), ((SUB, z.cols), i32),
         ((NPTS * NPTS, LANES), f32)],
        (VMEM,) * 3, (raw, refs, own_source), [VMEM((z.nv, width, LANES), f32)], flops=10**8, nbytes=4 * 10**6,
    )
    axes = ("elem", "lev")
    spread, to_far, to_near = call(
        serve_kernel, z,
        [((lax.axis_size(axes), 1, z.tracers), f32), ((z.part, LANES), f32), ((z.part, LANES), f32)],
        (VMEM,) * 5, (wown, in_far, in_near, sums, parts), [VMEM((REFS, LANES), f32)], flops=10**7, nbytes=3 * 10**6,
    )
    from_far = lax.ppermute(to_far, "elem", far)
    from_near = lax.ppermute(to_near, "elem", near)
    every = lax.all_to_all(spread, axes, 0, 0)
    (shaped,) = call(
        final_kernel, z,
        [((elems, levels, width), f32)],
        (VMEM,) * 5, (own, from_far, from_near, codes, coef),
        [VMEM((z.nv, width, LANES), f32), VMEM((z.nv, LANES, LANES), f32), VMEM(*flat), pltpu.SemaphoreType.DMA((z.tiles,))],
        flops=10**8, nbytes=3 * 10**6,
    )
    global_mass = every.sum(axis=(0, 1))
    whole_weight = 36.0 * 4.0 * elems * count * levels * lax.axis_size("lev")
    factor = target_mean * whole_weight / global_mass
    return shaped * jnp.repeat(factor, NPTS)[None, None, :]


def solution(mesh):
    placed = (P("elem", "lev", None), P("elem", None), P("elem", None, None), P("elem"), P())

    return jax.shard_map(per_device, mesh=mesh, in_specs=placed, out_specs=P("elem", "lev", None), check_vma=False)
```

```python
import functools
import math

import jax
import jax.numpy as jnp
import numpy as np
from jax import lax
from jax.experimental import pallas as pl
from jax.experimental.pallas import tpu as pltpu
from jax.sharding import PartitionSpec as P


NPTS = 16
REFS = 64
LANES = 128
SUB = 8

VMEM = pltpu.VMEM
SMEM = pltpu.SMEM


def lagrange_1d():
    side = math.isqrt(REFS)
    nodes = [np.float32(v) for v in (-1.0, -math.sqrt(0.2), math.sqrt(0.2), 1.0)]
    points = (-1.0 + 2.0 * np.arange(side, dtype=np.float32) / np.float32(side - 1)).astype(np.float32)
    columns = []
    for which in range(4):
        basis = np.ones((side,), np.float32)
        for other in range(4):
            if other != which:
                basis = basis * (points - nodes[other]) / (nodes[which] - nodes[other])
        columns.append(basis)
    return np.stack(columns, axis=1)


SIDE = math.isqrt(REFS)
BASIS = lagrange_1d()
WEIGHT36 = [ci * cj for ci in (1, 5, 5, 1) for cj in (1, 5, 5, 1)]


def split3(x):
    a = x.astype(jnp.bfloat16)
    rest = x - a.astype(jnp.float32)
    b = rest.astype(jnp.bfloat16)
    c = (rest - b.astype(jnp.float32)).astype(jnp.bfloat16)
    return a, b, c


def onehot_dot(parts, onehot):
    return sum(jnp.dot(part, onehot, preferred_element_type=jnp.float32) for part in parts)


def mm_nt(a, b):
    return lax.dot_general(a, b, (((1,), (1,)), ((), ())), preferred_element_type=jnp.float32)


class Sizes:
    def __init__(self, elems, levels, width, slots):
        self.elems, self.levels, self.width, self.slots = elems, levels, width, slots
        self.tracers = width // NPTS
        self.per = LANES // elems
        self.nv = levels // self.per
        self.cols = levels * elems
        self.tiles = width // LANES
        self.tpt = LANES // NPTS
        self.halves = LANES // (levels * slots)
        self.part = width // self.halves
        self.wrows = REFS // self.per


def plan_kernel(
    z, req_hbm, ref_hbm, src_hbm, wown_ref, far_ref, near_ref, ref_ref, src_ref, req_ref, sem
):
    elems, slots = z.elems, z.slots
    copies = [
        pltpu.make_async_copy(src, dst, sem.at[i])
        for i, (src, dst) in enumerate(((req_hbm, req_ref), (ref_hbm, ref_ref), (src_hbm, src_ref)))
    ]
    for copy in copies:
        copy.start()
    odd = lax.rem(lax.axis_index("elem"), 2)
    lane = lax.broadcasted_iota(jnp.int32, (1, LANES), 1)
    group = lane // elems
    row = lax.broadcasted_iota(jnp.int32, (z.wrows, LANES), 0) + z.wrows * group
    srow = lax.broadcasted_iota(jnp.int32, (LANES, LANES), 0)
    k_lane = lane % slots
    for copy in copies:
        copy.wait()
    ref = jnp.concatenate([ref_ref[...]] * z.per, axis=1)
    counts = tree(jnp.add, [jnp.where(row == ref[p : p + 1, :], float(WEIGHT36[p]), 0.0) for p in range(NPTS)])
    counts = counts.astype(jnp.bfloat16)
    src = jnp.concatenate([src_ref[...]] * z.per, axis=1)
    far_base, near_base = elems + odd * slots, elems + (1 - odd) * slots
    far = jnp.full((1, LANES), -1, jnp.int32)
    near = far
    pat_far = jnp.zeros((1, LANES), jnp.int32)
    pat_near = pat_far
    for k in range(slots):
        far_k, near_k = req_ref[0, odd, k], req_ref[0, 1 - odd, k]
        far = jnp.where(src == far_base + k, far_k, far)
        near = jnp.where(src == near_base + k, near_k, near)
        pat_far = jnp.where(k_lane == k, far_k, pat_far)
        pat_near = jnp.where(k_lane == k, near_k, pat_near)
    own = jnp.where(src < elems, src, -1)

    def weights(which):
        pick = srow == jnp.where(which >= 0, which + elems * group, -1)
        return mm_nt(counts, pick.astype(jnp.float32).astype(jnp.bfloat16))

    far_ref[0 : z.wrows, :] = weights(far)
    far_ref[z.wrows :, :] = jnp.broadcast_to(pat_far.astype(jnp.float32), (SUB, LANES))
    near_ref[0 : z.wrows, :] = weights(near)
    near_ref[z.wrows :, :] = jnp.broadcast_to(pat_near.astype(jnp.float32), (SUB, LANES))
    wown_ref[...] = weights(own)


def tables(z, src, ref, codes_ref, coef_ref):
    elems, slots, levels = z.elems, z.slots, z.levels
    odd = lax.rem(lax.axis_index("elem"), 2)
    lane = lax.broadcasted_iota(jnp.int32, (1, LANES), 1)
    src2 = jnp.concatenate([src] * z.per, axis=1)
    sub_level = lane // elems
    for v in range(z.nv):
        level = sub_level + v * z.per
        at = slice(v * LANES, (v + 1) * LANES)
        codes_ref[0:1, at] = jnp.where(src2 < elems, level * elems + src2, -1)
        rel = src2 - elems
        side = jnp.where(rel >= slots, 1, 0)
        code = jnp.where(side == odd, 0, LANES) + level * slots + (rel - side * slots)
        for h in range(z.halves):
            codes_ref[1 + h : 2 + h, at] = jnp.where(rel >= 0, code + h * levels * slots, -1)

    ref2 = jnp.concatenate([ref] * z.per, axis=1)
    one, two = ref2 // SIDE, ref2 % SIDE

    def basis(which):
        found = []
        for i in range(4):
            value = jnp.zeros(which.shape, jnp.float32)
            for a in range(SIDE):
                if BASIS[a, i] != 0.0:
                    value = jnp.where(which == a, float(BASIS[a, i]), value)
            found.append(value)
        return found

    la, lb = basis(one), basis(two)
    for i in range(4):
        for j in range(4):
            n = 4 * i + j
            coef_ref[n * NPTS : (n + 1) * NPTS, :] = la[i] * lb[j]


def line(x):
    out = [None] * SIDE
    out[0], out[SIDE - 1] = x[0], x[3]
    outer, inner = x[0] + x[3], x[1] + x[2]
    outer_odd, inner_odd = x[0] - x[3], x[1] - x[2]
    for a in range(1, SIDE // 2):
        c = [float(v) for v in BASIS[a]]
        even = (0.5 * (c[0] + c[3])) * outer + (0.5 * (c[1] + c[2])) * inner
        odd = (0.5 * (c[0] - c[3])) * outer_odd + (0.5 * (c[1] - c[2])) * inner_odd
        out[a], out[SIDE - 1 - a] = even + odd, even - odd
    return out


def tree(op, values):
    while len(values) > 1:
        values = [op(values[i], values[i + 1]) if i + 1 < len(values) else values[i] for i in range(0, len(values), 2)]
    return values[0]


def prep_kernel(z, x_ref, ref_ref, src_ref, parts_ref, own_ref, sums_ref, codes_ref, coef_ref, xt_ref):
    tables(z, src_ref[...], ref_ref[...], codes_ref, coef_ref)
    for j in range(z.tiles):
        for v in range(z.nv):
            rows = []
            for q in range(z.per):
                level = v * z.per + q
                for e in range(0, z.elems, SUB):
                    rows.append(x_ref[pl.ds(e, SUB), level, pl.ds(j * LANES, LANES)])
            block = jnp.concatenate(rows, axis=0)
            xt_ref[v, j * LANES : (j + 1) * LANES, :] = block.T
    a, b, c = split3(jnp.concatenate([xt_ref[v] for v in range(z.nv)], axis=1))
    parts_ref[0], parts_ref[1], parts_ref[2] = a, b, c
    row = lax.broadcasted_iota(jnp.int32, (z.cols, z.cols), 0)
    pick = (row == codes_ref[0:1, :]).astype(jnp.float32).astype(jnp.bfloat16)
    own_ref[...] = onehot_dot((a, b, c), pick)
    for j in range(z.tiles):
        both = [None] * REFS
        for v in range(z.nv):
            x = [xt_ref[v, pl.ds(j * LANES + n, z.tpt, stride=NPTS), :] for n in range(NPTS)]
            lowest, highest = tree(jnp.minimum, x), tree(jnp.maximum, x)
            lines = [line(x[4 * i : 4 * i + 4]) for i in range(4)]
            for b in range(SIDE):
                column = line([lines[i][b] for i in range(4)])
                for a in range(SIDE):
                    value = jnp.minimum(jnp.maximum(column[a], lowest), highest)
                    r = a * SIDE + b
                    both[r] = value if both[r] is None else both[r] + value
        low = lax.broadcasted_iota(jnp.int32, (1, LANES), 1) < z.elems
        for r in range(z.wrows):
            one, two = both[r], both[r + z.wrows]
            folded = jnp.where(low, one, two) + pltpu.roll(jnp.where(low, two, one), z.elems, 1)
            sums_ref[r * z.tracers + j * z.tpt : r * z.tracers + (j + 1) * z.tpt, :] = folded


def serve_kernel(
    z, wown_ref, infar_ref, innear_ref, sums_ref, parts_ref, spread_hbm, tofar_ref, tonear_ref, weight_ref, mass_ref, sem
):
    weight_ref[...] = wown_ref[...] + infar_ref[0 : z.wrows, :] + innear_ref[0 : z.wrows, :]
    total = [None] * z.tiles
    for r in range(z.wrows):
        w = weight_ref[pl.ds(r, 1), :]
        for j in range(z.tiles):
            lo = r * z.tracers + j * z.tpt
            term = sums_ref[lo : lo + z.tpt, :] * w
            total[j] = term if total[j] is None else total[j] + term
    total = jnp.concatenate(total, axis=0)
    ones = jnp.ones((SUB, LANES), jnp.bfloat16)
    mass = sum(mm_nt(ones, part) for part in split3(total))[0:1, :]
    mass_ref[...] = jnp.broadcast_to(mass[None], mass_ref.shape)
    copy = pltpu.make_async_copy(mass_ref, spread_hbm, sem)
    copy.start()
    lane = lax.broadcasted_iota(jnp.int32, (1, LANES), 1)
    level = (lane // z.slots) % z.levels
    codes = []
    for ref in (infar_ref, innear_ref):
        wanted = ref[z.wrows : z.wrows + 1, :].astype(jnp.int32)
        codes.append(jnp.where(wanted >= 0, level * z.elems + wanted, -1))
    code = jnp.concatenate(codes, axis=1)
    row = lax.broadcasted_iota(jnp.int32, (z.cols, 2 * LANES), 0)
    pick = (row == code).astype(jnp.float32).astype(jnp.bfloat16)
    rows = onehot_dot((parts_ref[0], parts_ref[1], parts_ref[2]), pick)
    half = lane // (z.levels * z.slots)
    for ref, at in ((tofar_ref, slice(0, LANES)), (tonear_ref, slice(LANES, 2 * LANES))):
        value = rows[0 : z.part, at]
        for h in range(1, z.halves):
            value = jnp.where(half == h, rows[h * z.part : (h + 1) * z.part, at], value)
        ref[...] = value
    copy.wait()


def final_kernel(z, own_ref, far_ref, near_ref, codes_ref, coef_ref, out_ref, got_ref, turn_ref, flat_ref, sem):
    halo = jnp.concatenate([far_ref[...], near_ref[...]], axis=1)
    parts = split3(halo)
    row = lax.broadcasted_iota(jnp.int32, (2 * LANES, z.cols), 0)
    for h in range(z.halves):
        pick = (row == codes_ref[1 + h : 2 + h, :]).astype(jnp.float32).astype(jnp.bfloat16)
        at = slice(h * z.part, (h + 1) * z.part)
        got = own_ref[at, :] + onehot_dot(parts, pick)
        for v in range(z.nv):
            got_ref[v, at, :] = got[:, v * LANES : (v + 1) * LANES]
    copies = []
    for j in range(z.tiles):
        xs, low, high = [], [], []
        for v in range(z.nv):
            x = [got_ref[v, pl.ds(j * LANES + n, z.tpt, stride=NPTS), :] for n in range(NPTS)]
            xs.append(x)
            low.append(tree(jnp.minimum, x))
            high.append(tree(jnp.maximum, x))
        for p in range(NPTS):
            coef = [coef_ref[pl.ds(n * NPTS + p, 1), :] for n in range(NPTS)]
            for v in range(z.nv):
                value = tree(jnp.add, [coef[n] * xs[v][n] for n in range(NPTS)])
                value = jnp.minimum(jnp.maximum(value, low[v]), high[v])
                turn_ref[v, pl.ds(p, z.tpt, stride=NPTS), :] = value
        for v in range(z.nv):
            block = turn_ref[v].T
            for q in range(z.per):
                level = v * z.per + q
                for e in range(0, z.elems, SUB):
                    piece = block[q * z.elems + e : q * z.elems + e + SUB, :]
                    flat_ref[j, pl.ds(e * z.levels + level, SUB, stride=z.levels), :] = piece
        copies.append(
            pltpu.make_async_copy(
                flat_ref.at[j].reshape(z.elems, z.levels, LANES), out_ref.at[:, :, pl.ds(j * LANES, LANES)], sem.at[j]
            )
        )
        copies[-1].start()
    for copy in copies:
        copy.wait()


def in_hbm(x):
    return pltpu.with_memory_space_constraint(x, pltpu.HBM)


def call(kernel, z, outs, ins, args, scratch=(), flops=0, nbytes=0, limit=16, spaces=None):
    return pl.pallas_call(
        functools.partial(kernel, z),
        out_shape=[jax.ShapeDtypeStruct(shape, dtype) for shape, dtype in outs],
        in_specs=[pl.BlockSpec(memory_space=space) for space in ins],
        out_specs=[pl.BlockSpec(memory_space=space) for space in spaces or [VMEM] * len(outs)],
        scratch_shapes=list(scratch),
        cost_estimate=pl.CostEstimate(flops=flops, bytes_accessed=nbytes, transcendentals=0),
        compiler_params=pltpu.CompilerParams(vmem_limit_bytes=limit << 20),
    )(*args)


def per_device(tracers, ref_index, requests, source, target_mean):
    elems, levels, width = tracers.shape
    z = Sizes(elems, levels, width, requests.shape[2])
    assert z.per == 2 and z.per * elems == LANES and z.nv * z.per == levels and z.tiles * LANES == width
    assert z.halves * levels * z.slots == LANES and z.part * z.halves == width
    f32, bf16, i32 = jnp.float32, jnp.bfloat16, jnp.int32
    flat = ((z.tiles, elems * levels, LANES), f32)
    wown, ask_far, ask_near, refs, own_source = call(
        plan_kernel, z,
        [((z.wrows, LANES), f32), ((z.wrows + SUB, LANES), f32), ((z.wrows + SUB, LANES), f32),
         ((NPTS, elems), i32), ((1, elems), i32)],
        (pltpu.HBM,) * 3, [in_hbm(a) for a in (requests, ref_index.T, source.reshape(1, elems))],
        [SMEM(requests.shape, i32), pltpu.SemaphoreType.DMA((3,))],
        flops=10**9, nbytes=10**7,
    )
    count = lax.axis_size("elem")
    assert count % 2 == 0
    far = [(i, (i - 1 if i % 2 == 0 else i + 1) % count) for i in range(count)]
    near = [(i, i + 1 if i % 2 == 0 else i - 1) for i in range(count)]
    in_far = lax.ppermute(ask_far, "elem", far)
    in_near = lax.ppermute(ask_near, "elem", near)
    parts, own, sums, codes, coef = call(
        prep_kernel, z,
        [((3, width, z.cols), bf16), ((width, z.cols), f32), ((z.wrows * z.tracers, LANES), f32), ((SUB, z.cols), i32),
         ((NPTS * NPTS, LANES), f32)],
        (VMEM, VMEM, VMEM), (tracers, refs, own_source),
        [VMEM((z.nv, width, LANES), f32)], flops=10**8, nbytes=4 * 10**6,
    )
    axes = ("elem", "lev")
    spread_shape = ((lax.axis_size(axes), 1, z.tracers), f32)
    spread, to_far, to_near = call(
        serve_kernel, z,
        [spread_shape, ((z.part, LANES), f32), ((z.part, LANES), f32)],
        (VMEM,) * 5, (wown, in_far, in_near, sums, parts),
        [VMEM((z.wrows, LANES), f32), VMEM(*spread_shape), pltpu.SemaphoreType.DMA(())],
        flops=10**7, nbytes=3 * 10**6, spaces=(pltpu.HBM, VMEM, VMEM),
    )
    from_far = lax.ppermute(to_far, "elem", far)
    from_near = lax.ppermute(to_near, "elem", near)
    every = lax.all_to_all(spread, axes, 0, 0)
    (shaped,) = call(
        final_kernel, z,
        [((elems, levels, width), f32)],
        (VMEM,) * 5, (own, from_far, from_near, codes, coef),
        [VMEM((z.nv, width, LANES), f32), VMEM((z.nv, LANES, LANES), f32), VMEM(*flat), pltpu.SemaphoreType.DMA((z.tiles,))],
        flops=10**8, nbytes=3 * 10**6,
    )
    global_mass = every.sum(axis=(0, 1))
    whole_weight = 36.0 * 4.0 * elems * count * levels * lax.axis_size("lev")
    factor = target_mean * whole_weight / global_mass
    return shaped * jnp.repeat(factor, NPTS)[None, None, :]


def solution(mesh):
    placed = (P("elem", "lev", None), P("elem", None), P("elem", None, None), P("elem"), P())

    return jax.shard_map(per_device, mesh=mesh, in_specs=placed, out_specs=P("elem", "lev", None), check_vma=False)
```

```python
import functools
import math

import jax
import jax.numpy as jnp
import numpy as np
from jax import lax
from jax.experimental import pallas as pl
from jax.experimental.pallas import tpu as pltpu
from jax.sharding import PartitionSpec as P


NPTS = 16
REFS = 64
LANES = 128
SUB = 8

VMEM = pltpu.VMEM
SMEM = pltpu.SMEM


def lagrange_1d():
    side = math.isqrt(REFS)
    nodes = [np.float32(v) for v in (-1.0, -math.sqrt(0.2), math.sqrt(0.2), 1.0)]
    points = (-1.0 + 2.0 * np.arange(side, dtype=np.float32) / np.float32(side - 1)).astype(np.float32)
    columns = []
    for which in range(4):
        basis = np.ones((side,), np.float32)
        for other in range(4):
            if other != which:
                basis = basis * (points - nodes[other]) / (nodes[which] - nodes[other])
        columns.append(basis)
    return np.stack(columns, axis=1)


SIDE = math.isqrt(REFS)
BASIS = lagrange_1d()
WEIGHT36 = [ci * cj for ci in (1, 5, 5, 1) for cj in (1, 5, 5, 1)]


def split3(x):
    a = x.astype(jnp.bfloat16)
    rest = x - a.astype(jnp.float32)
    b = rest.astype(jnp.bfloat16)
    c = (rest - b.astype(jnp.float32)).astype(jnp.bfloat16)
    return a, b, c


def onehot_dot(parts, onehot):
    return sum(jnp.dot(part, onehot, preferred_element_type=jnp.float32) for part in parts)


def mm_nt(a, b):
    return lax.dot_general(a, b, (((1,), (1,)), ((), ())), preferred_element_type=jnp.float32)


class Sizes:
    def __init__(self, elems, levels, width, slots):
        self.elems, self.levels, self.width, self.slots = elems, levels, width, slots
        self.tracers = width // NPTS
        self.per = LANES // elems
        self.nv = levels // self.per
        self.cols = levels * elems
        self.tiles = width // LANES
        self.tpt = LANES // NPTS
        self.halves = LANES // (levels * slots)
        self.part = width // self.halves
        self.wrows = REFS // self.per


def plan_kernel(
    z, req_hbm, ref_hbm, src_hbm, wown_ref, far_ref, near_ref, ref_ref, src_ref, req_ref, sem
):
    elems, slots = z.elems, z.slots
    copies = [
        pltpu.make_async_copy(src, dst, sem.at[i])
        for i, (src, dst) in enumerate(((req_hbm, req_ref), (ref_hbm, ref_ref), (src_hbm, src_ref)))
    ]
    for copy in copies:
        copy.start()
    odd = lax.rem(lax.axis_index("elem"), 2)
    lane = lax.broadcasted_iota(jnp.int32, (1, LANES), 1)
    group = lane // elems
    row = lax.broadcasted_iota(jnp.int32, (z.wrows, LANES), 0) + z.wrows * group
    srow = lax.broadcasted_iota(jnp.int32, (LANES, LANES), 0)
    k_lane = lane % slots
    for copy in copies:
        copy.wait()
    ref = jnp.concatenate([ref_ref[...]] * z.per, axis=1)
    counts = tree(jnp.add, [jnp.where(row == ref[p : p + 1, :], float(WEIGHT36[p]), 0.0) for p in range(NPTS)])
    counts = counts.astype(jnp.bfloat16)
    src = jnp.concatenate([src_ref[...]] * z.per, axis=1)
    far_base, near_base = elems + odd * slots, elems + (1 - odd) * slots
    far = jnp.full((1, LANES), -1, jnp.int32)
    near = far
    pat_far = jnp.zeros((1, LANES), jnp.int32)
    pat_near = pat_far
    for k in range(slots):
        far_k, near_k = req_ref[0, odd, k], req_ref[0, 1 - odd, k]
        far = jnp.where(src == far_base + k, far_k, far)
        near = jnp.where(src == near_base + k, near_k, near)
        pat_far = jnp.where(k_lane == k, far_k, pat_far)
        pat_near = jnp.where(k_lane == k, near_k, pat_near)
    own = jnp.where(src < elems, src, -1)

    def weights(which):
        pick = srow == jnp.where(which >= 0, which + elems * group, -1)
        return mm_nt(counts, pick.astype(jnp.float32).astype(jnp.bfloat16))

    far_ref[0 : z.wrows, :] = weights(far)
    far_ref[z.wrows :, :] = jnp.broadcast_to(pat_far.astype(jnp.float32), (SUB, LANES))
    near_ref[0 : z.wrows, :] = weights(near)
    near_ref[z.wrows :, :] = jnp.broadcast_to(pat_near.astype(jnp.float32), (SUB, LANES))
    wown_ref[...] = weights(own)


def tables(z, src, ref, codes_ref, coef_ref):
    elems, slots, levels = z.elems, z.slots, z.levels
    odd = lax.rem(lax.axis_index("elem"), 2)
    lane = lax.broadcasted_iota(jnp.int32, (1, LANES), 1)
    src2 = jnp.concatenate([src] * z.per, axis=1)
    sub_level = lane // elems
    for v in range(z.nv):
        level = sub_level + v * z.per
        at = slice(v * LANES, (v + 1) * LANES)
        codes_ref[0:1, at] = jnp.where(src2 < elems, level * elems + src2, -1)
        rel = src2 - elems
        side = jnp.where(rel >= slots, 1, 0)
        code = jnp.where(side == odd, 0, LANES) + level * slots + (rel - side * slots)
        for h in range(z.halves):
            codes_ref[1 + h : 2 + h, at] = jnp.where(rel >= 0, code + h * levels * slots, -1)

    ref2 = jnp.concatenate([ref] * z.per, axis=1)
    one, two = ref2 // SIDE, ref2 % SIDE

    def basis(which):
        found = []
        for i in range(4):
            value = jnp.zeros(which.shape, jnp.float32)
            for a in range(SIDE):
                if BASIS[a, i] != 0.0:
                    value = jnp.where(which == a, float(BASIS[a, i]), value)
            found.append(value)
        return found

    la, lb = basis(one), basis(two)
    for i in range(4):
        for j in range(4):
            n = 4 * i + j
            coef_ref[n * NPTS : (n + 1) * NPTS, :] = la[i] * lb[j]


def line(x):
    out = [None] * SIDE
    out[0], out[SIDE - 1] = x[0], x[3]
    outer, inner = x[0] + x[3], x[1] + x[2]
    outer_odd, inner_odd = x[0] - x[3], x[1] - x[2]
    for a in range(1, SIDE // 2):
        c = [float(v) for v in BASIS[a]]
        even = (0.5 * (c[0] + c[3])) * outer + (0.5 * (c[1] + c[2])) * inner
        odd = (0.5 * (c[0] - c[3])) * outer_odd + (0.5 * (c[1] - c[2])) * inner_odd
        out[a], out[SIDE - 1 - a] = even + odd, even - odd
    return out


def tree(op, values):
    while len(values) > 1:
        values = [op(values[i], values[i + 1]) if i + 1 < len(values) else values[i] for i in range(0, len(values), 2)]
    return values[0]


def prep_kernel(z, x_ref, ref_ref, src_ref, parts_ref, own_ref, sums_ref, codes_ref, coef_ref, xt_ref):
    tables(z, src_ref[...], ref_ref[...], codes_ref, coef_ref)
    for j in range(z.tiles):
        for v in range(z.nv):
            rows = []
            for q in range(z.per):
                level = v * z.per + q
                for e in range(0, z.elems, SUB):
                    rows.append(x_ref[pl.ds(e, SUB), level, pl.ds(j * LANES, LANES)])
            block = jnp.concatenate(rows, axis=0)
            xt_ref[v, j * LANES : (j + 1) * LANES, :] = block.T
    a, b, c = split3(jnp.concatenate([xt_ref[v] for v in range(z.nv)], axis=1))
    parts_ref[0], parts_ref[1], parts_ref[2] = a, b, c
    row = lax.broadcasted_iota(jnp.int32, (z.cols, z.cols), 0)
    pick = (row == codes_ref[0:1, :]).astype(jnp.float32).astype(jnp.bfloat16)
    own_ref[...] = onehot_dot((a, b, c), pick)
    for j in range(z.tiles):
        both = [None] * REFS
        for v in range(z.nv):
            x = [xt_ref[v, pl.ds(j * LANES + n, z.tpt, stride=NPTS), :] for n in range(NPTS)]
            lowest, highest = tree(jnp.minimum, x), tree(jnp.maximum, x)
            lines = [line(x[4 * i : 4 * i + 4]) for i in range(4)]
            for b in range(SIDE):
                column = line([lines[i][b] for i in range(4)])
                for a in range(SIDE):
                    value = jnp.minimum(jnp.maximum(column[a], lowest), highest)
                    r = a * SIDE + b
                    both[r] = value if both[r] is None else both[r] + value
        low = lax.broadcasted_iota(jnp.int32, (1, LANES), 1) < z.elems
        for r in range(z.wrows):
            one, two = both[r], both[r + z.wrows]
            folded = jnp.where(low, one, two) + pltpu.roll(jnp.where(low, two, one), z.elems, 1)
            sums_ref[r * z.tracers + j * z.tpt : r * z.tracers + (j + 1) * z.tpt, :] = folded


def serve_kernel(
    z, wown_ref, infar_ref, innear_ref, sums_ref, parts_ref, spread_hbm, tofar_ref, tonear_ref, weight_ref, mass_ref, sem
):
    weight_ref[...] = wown_ref[...] + infar_ref[0 : z.wrows, :] + innear_ref[0 : z.wrows, :]
    total = [None] * z.tiles
    for r in range(z.wrows):
        w = weight_ref[pl.ds(r, 1), :]
        for j in range(z.tiles):
            lo = r * z.tracers + j * z.tpt
            term = sums_ref[lo : lo + z.tpt, :] * w
            total[j] = term if total[j] is None else total[j] + term
    total = jnp.concatenate(total, axis=0)
    ones = jnp.ones((SUB, LANES), jnp.bfloat16)
    mass = sum(mm_nt(ones, part) for part in split3(total))[0:1, :]
    mass_ref[...] = jnp.broadcast_to(mass[None], mass_ref.shape)
    copy = pltpu.make_async_copy(mass_ref, spread_hbm, sem)
    copy.start()
    lane = lax.broadcasted_iota(jnp.int32, (1, LANES), 1)
    level = (lane // z.slots) % z.levels
    codes = []
    for ref in (infar_ref, innear_ref):
        wanted = ref[z.wrows : z.wrows + 1, :].astype(jnp.int32)
        codes.append(jnp.where(wanted >= 0, level * z.elems + wanted, -1))
    code = jnp.concatenate(codes, axis=1)
    row = lax.broadcasted_iota(jnp.int32, (z.cols, 2 * LANES), 0)
    pick = (row == code).astype(jnp.float32).astype(jnp.bfloat16)
    rows = onehot_dot((parts_ref[0], parts_ref[1], parts_ref[2]), pick)
    half = lane // (z.levels * z.slots)
    for ref, at in ((tofar_ref, slice(0, LANES)), (tonear_ref, slice(LANES, 2 * LANES))):
        value = rows[0 : z.part, at]
        for h in range(1, z.halves):
            value = jnp.where(half == h, rows[h * z.part : (h + 1) * z.part, at], value)
        ref[...] = value
    copy.wait()


def final_kernel(z, own_ref, far_ref, near_ref, codes_ref, coef_ref, flat_ref, got_ref, turn_ref):
    halo = jnp.concatenate([far_ref[...], near_ref[...]], axis=1)
    parts = split3(halo)
    row = lax.broadcasted_iota(jnp.int32, (2 * LANES, z.cols), 0)
    for h in range(z.halves):
        pick = (row == codes_ref[1 + h : 2 + h, :]).astype(jnp.float32).astype(jnp.bfloat16)
        at = slice(h * z.part, (h + 1) * z.part)
        got = own_ref[at, :] + onehot_dot(parts, pick)
        for v in range(z.nv):
            got_ref[v, at, :] = got[:, v * LANES : (v + 1) * LANES]
    for j in range(z.tiles):
        xs, low, high = [], [], []
        for v in range(z.nv):
            x = [got_ref[v, pl.ds(j * LANES + n, z.tpt, stride=NPTS), :] for n in range(NPTS)]
            xs.append(x)
            low.append(tree(jnp.minimum, x))
            high.append(tree(jnp.maximum, x))
        for p in range(NPTS):
            coef = [coef_ref[pl.ds(n * NPTS + p, 1), :] for n in range(NPTS)]
            for v in range(z.nv):
                value = tree(jnp.add, [coef[n] * xs[v][n] for n in range(NPTS)])
                value = jnp.minimum(jnp.maximum(value, low[v]), high[v])
                turn_ref[v, pl.ds(p, z.tpt, stride=NPTS), :] = value
        for v in range(z.nv):
            block = turn_ref[v].T
            for q in range(z.per):
                level = v * z.per + q
                for e in range(0, z.elems, SUB):
                    piece = block[q * z.elems + e : q * z.elems + e + SUB, :]
                    flat_ref[j, pl.ds(e * z.levels + level, SUB, stride=z.levels), :] = piece


def scale_kernel(z, whole_weight, every_ref, mean_ref, flat_ref, out_hbm, stage_ref, sem):
    total = tree(jnp.add, [every_ref[m] for m in range(every_ref.shape[0])])
    factor = mean_ref[...] * whole_weight / total
    factor = jnp.concatenate([factor, jnp.zeros((1, LANES - z.tracers), jnp.float32)], axis=1)
    factor = jnp.broadcast_to(factor, (SUB, LANES))
    lane = lax.broadcasted_iota(jnp.int32, (SUB, LANES), 1)
    copies = []
    for j in range(z.tiles):
        mine = jnp.take_along_axis(factor, j * z.tpt + lane // NPTS, axis=1)
        stage_ref[j] = flat_ref[j] * mine[0:1, :]
        copies.append(
            pltpu.make_async_copy(
                stage_ref.at[j].reshape(z.elems, z.levels, LANES), out_hbm.at[:, :, pl.ds(j * LANES, LANES)], sem.at[j]
            )
        )
        copies[-1].start()
    for copy in copies:
        copy.wait()


def in_hbm(x):
    return pltpu.with_memory_space_constraint(x, pltpu.HBM)


def call(kernel, z, outs, ins, args, scratch=(), flops=0, nbytes=0, limit=16, spaces=None):
    return pl.pallas_call(
        functools.partial(kernel, z),
        out_shape=[jax.ShapeDtypeStruct(shape, dtype) for shape, dtype in outs],
        in_specs=[pl.BlockSpec(memory_space=space) for space in ins],
        out_specs=[pl.BlockSpec(memory_space=space) for space in spaces or [VMEM] * len(outs)],
        scratch_shapes=list(scratch),
        cost_estimate=pl.CostEstimate(flops=flops, bytes_accessed=nbytes, transcendentals=0),
        compiler_params=pltpu.CompilerParams(vmem_limit_bytes=limit << 20),
    )(*args)


def per_device(tracers, ref_index, requests, source, target_mean):
    elems, levels, width = tracers.shape
    z = Sizes(elems, levels, width, requests.shape[2])
    assert z.per == 2 and z.per * elems == LANES and z.nv * z.per == levels and z.tiles * LANES == width
    assert z.halves * levels * z.slots == LANES and z.part * z.halves == width
    f32, bf16, i32 = jnp.float32, jnp.bfloat16, jnp.int32
    flat = ((z.tiles, elems * levels, LANES), f32)
    wown, ask_far, ask_near, refs, own_source = call(
        plan_kernel, z,
        [((z.wrows, LANES), f32), ((z.wrows + SUB, LANES), f32), ((z.wrows + SUB, LANES), f32),
         ((NPTS, elems), i32), ((1, elems), i32)],
        (pltpu.HBM,) * 3, [in_hbm(a) for a in (requests, ref_index.T, source.reshape(1, elems))],
        [SMEM(requests.shape, i32), pltpu.SemaphoreType.DMA((3,))],
        flops=10**9, nbytes=10**7,
    )
    count = lax.axis_size("elem")
    assert count % 2 == 0
    far = [(i, (i - 1 if i % 2 == 0 else i + 1) % count) for i in range(count)]
    near = [(i, i + 1 if i % 2 == 0 else i - 1) for i in range(count)]
    in_far = lax.ppermute(ask_far, "elem", far)
    in_near = lax.ppermute(ask_near, "elem", near)
    parts, own, sums, codes, coef = call(
        prep_kernel, z,
        [((3, width, z.cols), bf16), ((width, z.cols), f32), ((z.wrows * z.tracers, LANES), f32), ((SUB, z.cols), i32),
         ((NPTS * NPTS, LANES), f32)],
        (VMEM, VMEM, VMEM), (tracers, refs, own_source),
        [VMEM((z.nv, width, LANES), f32)], flops=10**8, nbytes=4 * 10**6,
    )
    axes = ("elem", "lev")
    spread_shape = ((lax.axis_size(axes), 1, z.tracers), f32)
    spread, to_far, to_near = call(
        serve_kernel, z,
        [spread_shape, ((z.part, LANES), f32), ((z.part, LANES), f32)],
        (VMEM,) * 5, (wown, in_far, in_near, sums, parts),
        [VMEM((z.wrows, LANES), f32), VMEM(*spread_shape), pltpu.SemaphoreType.DMA(())],
        flops=10**7, nbytes=3 * 10**6, spaces=(pltpu.HBM, VMEM, VMEM),
    )
    from_far = lax.ppermute(to_far, "elem", far)
    from_near = lax.ppermute(to_near, "elem", near)
    every = lax.all_to_all(spread, axes, 0, 0)
    (shaped,) = call(
        final_kernel, z,
        [flat],
        (VMEM,) * 5, (own, from_far, from_near, codes, coef),
        [VMEM((z.nv, width, LANES), f32), VMEM((z.nv, LANES, LANES), f32)],
        flops=10**8, nbytes=3 * 10**6,
    )
    whole_weight = 36.0 * 4.0 * elems * count * levels * lax.axis_size("lev")
    (out,) = call(
        lambda z, *refs: scale_kernel(z, whole_weight, *refs), z,
        [((elems, levels, width), f32)],
        (VMEM,) * 3, (every, target_mean.reshape(1, z.tracers), shaped),
        [VMEM(*flat), pltpu.SemaphoreType.DMA((z.tiles,))], flops=10**6, nbytes=10**6, spaces=(pltpu.HBM,),
    )
    return out


def solution(mesh):
    placed = (P("elem", "lev", None), P("elem", None), P("elem", None, None), P("elem"), P())

    return jax.shard_map(per_device, mesh=mesh, in_specs=placed, out_specs=P("elem", "lev", None), check_vma=False)
```

```python
import functools
import math

import jax
import jax.numpy as jnp
import numpy as np
from jax import lax
from jax.experimental import pallas as pl
from jax.experimental.pallas import tpu as pltpu
from jax.sharding import PartitionSpec as P


NPTS = 16
REFS = 64
LANES = 128
SUB = 8

VMEM = pltpu.VMEM
SMEM = pltpu.SMEM


def lagrange_1d():
    side = math.isqrt(REFS)
    nodes = [np.float32(v) for v in (-1.0, -math.sqrt(0.2), math.sqrt(0.2), 1.0)]
    points = (-1.0 + 2.0 * np.arange(side, dtype=np.float32) / np.float32(side - 1)).astype(np.float32)
    columns = []
    for which in range(4):
        basis = np.ones((side,), np.float32)
        for other in range(4):
            if other != which:
                basis = basis * (points - nodes[other]) / (nodes[which] - nodes[other])
        columns.append(basis)
    return np.stack(columns, axis=1)


SIDE = math.isqrt(REFS)
BASIS = lagrange_1d()
WEIGHT36 = [ci * cj for ci in (1, 5, 5, 1) for cj in (1, 5, 5, 1)]


def split3(x):
    a = x.astype(jnp.bfloat16)
    rest = x - a.astype(jnp.float32)
    b = rest.astype(jnp.bfloat16)
    c = (rest - b.astype(jnp.float32)).astype(jnp.bfloat16)
    return a, b, c


def onehot_dot(parts, onehot):
    return sum(jnp.dot(part, onehot, preferred_element_type=jnp.float32) for part in parts)


def mm_nt(a, b):
    return lax.dot_general(a, b, (((1,), (1,)), ((), ())), preferred_element_type=jnp.float32)


class Sizes:
    def __init__(self, elems, levels, width, slots):
        self.elems, self.levels, self.width, self.slots = elems, levels, width, slots
        self.tracers = width // NPTS
        self.per = LANES // elems
        self.nv = levels // self.per
        self.cols = levels * elems
        self.tiles = width // LANES
        self.tpt = LANES // NPTS
        self.halves = LANES // (levels * slots)
        self.part = width // self.halves
        self.wrows = REFS // self.per


def plan_kernel(
    z, req_hbm, ref_hbm, src_hbm, wown_ref, far_ref, near_ref, ref_ref, src_ref, req_ref, sem
):
    elems, slots = z.elems, z.slots
    copies = [
        pltpu.make_async_copy(src, dst, sem.at[i])
        for i, (src, dst) in enumerate(((req_hbm, req_ref), (ref_hbm, ref_ref), (src_hbm, src_ref)))
    ]
    for copy in copies:
        copy.start()
    odd = lax.rem(lax.axis_index("elem"), 2)
    lane = lax.broadcasted_iota(jnp.int32, (1, LANES), 1)
    group = lane // elems
    row = lax.broadcasted_iota(jnp.int32, (z.wrows, LANES), 0) + z.wrows * group
    srow = lax.broadcasted_iota(jnp.int32, (LANES, LANES), 0)
    k_lane = lane % slots
    for copy in copies:
        copy.wait()
    ref = jnp.concatenate([ref_ref[...]] * z.per, axis=1)
    counts = tree(jnp.add, [jnp.where(row == ref[p : p + 1, :], float(WEIGHT36[p]), 0.0) for p in range(NPTS)])
    counts = counts.astype(jnp.bfloat16)
    src = jnp.concatenate([src_ref[...]] * z.per, axis=1)
    far_base, near_base = elems + odd * slots, elems + (1 - odd) * slots
    far = jnp.full((1, LANES), -1, jnp.int32)
    near = far
    pat_far = jnp.zeros((1, LANES), jnp.int32)
    pat_near = pat_far
    for k in range(slots):
        far_k, near_k = req_ref[0, odd, k], req_ref[0, 1 - odd, k]
        far = jnp.where(src == far_base + k, far_k, far)
        near = jnp.where(src == near_base + k, near_k, near)
        pat_far = jnp.where(k_lane == k, far_k, pat_far)
        pat_near = jnp.where(k_lane == k, near_k, pat_near)
    own = jnp.where(src < elems, src, -1)

    def weights(which):
        pick = srow == jnp.where(which >= 0, which + elems * group, -1)
        return mm_nt(counts, pick.astype(jnp.float32).astype(jnp.bfloat16))

    far_ref[0 : z.wrows, :] = weights(far)
    far_ref[z.wrows :, :] = jnp.broadcast_to(pat_far.astype(jnp.float32), (SUB, LANES))
    near_ref[0 : z.wrows, :] = weights(near)
    near_ref[z.wrows :, :] = jnp.broadcast_to(pat_near.astype(jnp.float32), (SUB, LANES))
    wown_ref[...] = weights(own)


def tables(z, src, ref, codes_ref, coef_ref):
    elems, slots, levels = z.elems, z.slots, z.levels
    odd = lax.rem(lax.axis_index("elem"), 2)
    lane = lax.broadcasted_iota(jnp.int32, (1, LANES), 1)
    src2 = jnp.concatenate([src] * z.per, axis=1)
    sub_level = lane // elems
    for v in range(z.nv):
        level = sub_level + v * z.per
        at = slice(v * LANES, (v + 1) * LANES)
        codes_ref[0:1, at] = jnp.where(src2 < elems, level * elems + src2, -1)
        rel = src2 - elems
        side = jnp.where(rel >= slots, 1, 0)
        code = jnp.where(side == odd, 0, LANES) + level * slots + (rel - side * slots)
        for h in range(z.halves):
            codes_ref[1 + h : 2 + h, at] = jnp.where(rel >= 0, code + h * levels * slots, -1)

    ref2 = jnp.concatenate([ref] * z.per, axis=1)
    one, two = ref2 // SIDE, ref2 % SIDE

    def basis(which):
        found = []
        for i in range(4):
            value = jnp.zeros(which.shape, jnp.float32)
            for a in range(SIDE):
                if BASIS[a, i] != 0.0:
                    value = jnp.where(which == a, float(BASIS[a, i]), value)
            found.append(value)
        return found

    la, lb = basis(one), basis(two)
    for i in range(4):
        for j in range(4):
            n = 4 * i + j
            coef_ref[n * NPTS : (n + 1) * NPTS, :] = la[i] * lb[j]


def line(x):
    out = [None] * SIDE
    out[0], out[SIDE - 1] = x[0], x[3]
    outer, inner = x[0] + x[3], x[1] + x[2]
    outer_odd, inner_odd = x[0] - x[3], x[1] - x[2]
    for a in range(1, SIDE // 2):
        c = [float(v) for v in BASIS[a]]
        even = (0.5 * (c[0] + c[3])) * outer + (0.5 * (c[1] + c[2])) * inner
        odd = (0.5 * (c[0] - c[3])) * outer_odd + (0.5 * (c[1] - c[2])) * inner_odd
        out[a], out[SIDE - 1 - a] = even + odd, even - odd
    return out


def tree(op, values):
    while len(values) > 1:
        values = [op(values[i], values[i + 1]) if i + 1 < len(values) else values[i] for i in range(0, len(values), 2)]
    return values[0]


def prep_kernel(z, x_ref, parts_ref, sums_ref, xt_ref):
    for j in range(z.tiles):
        for v in range(z.nv):
            rows = []
            for q in range(z.per):
                level = v * z.per + q
                for e in range(0, z.elems, SUB):
                    rows.append(x_ref[pl.ds(e, SUB), level, pl.ds(j * LANES, LANES)])
            block = jnp.concatenate(rows, axis=0)
            xt_ref[v, j * LANES : (j + 1) * LANES, :] = block.T
    a, b, c = split3(jnp.concatenate([xt_ref[v] for v in range(z.nv)], axis=1))
    parts_ref[0], parts_ref[1], parts_ref[2] = a, b, c
    for j in range(z.tiles):
        both = [None] * REFS
        for v in range(z.nv):
            x = [xt_ref[v, pl.ds(j * LANES + n, z.tpt, stride=NPTS), :] for n in range(NPTS)]
            lowest, highest = tree(jnp.minimum, x), tree(jnp.maximum, x)
            lines = [line(x[4 * i : 4 * i + 4]) for i in range(4)]
            for b in range(SIDE):
                column = line([lines[i][b] for i in range(4)])
                for a in range(SIDE):
                    value = jnp.minimum(jnp.maximum(column[a], lowest), highest)
                    r = a * SIDE + b
                    both[r] = value if both[r] is None else both[r] + value
        low = lax.broadcasted_iota(jnp.int32, (1, LANES), 1) < z.elems
        for r in range(z.wrows):
            one, two = both[r], both[r + z.wrows]
            folded = jnp.where(low, one, two) + pltpu.roll(jnp.where(low, two, one), z.elems, 1)
            sums_ref[r * z.tracers + j * z.tpt : r * z.tracers + (j + 1) * z.tpt, :] = folded


def serve_kernel(
    z, wown_ref, infar_ref, innear_ref, sums_ref, parts_ref, spread_hbm, tofar_ref, tonear_ref, weight_ref, mass_ref, sem
):
    weight_ref[...] = wown_ref[...] + infar_ref[0 : z.wrows, :] + innear_ref[0 : z.wrows, :]
    terms = [[] for _ in range(z.tiles)]
    for r in range(z.wrows):
        w = weight_ref[pl.ds(r, 1), :]
        for j in range(z.tiles):
            lo = r * z.tracers + j * z.tpt
            term = sums_ref[lo : lo + z.tpt, :] * w
            if len(terms[j]) < 4:
                terms[j].append(term)
            else:
                terms[j][r % 4] = terms[j][r % 4] + term
    total = jnp.concatenate([tree(jnp.add, parts) for parts in terms], axis=0)
    mass = jnp.sum(total.T, axis=0, keepdims=True)
    mass_ref[...] = jnp.broadcast_to(mass[None], mass_ref.shape)
    copy = pltpu.make_async_copy(mass_ref, spread_hbm, sem)
    copy.start()

    @pl.when(lax.axis_index("elem") >= 0)
    def _():
        lane = lax.broadcasted_iota(jnp.int32, (1, LANES), 1)
        level = (lane // z.slots) % z.levels
        codes = []
        for ref in (infar_ref, innear_ref):
            wanted = ref[z.wrows : z.wrows + 1, :].astype(jnp.int32)
            codes.append(jnp.where(wanted >= 0, level * z.elems + wanted, -1))
        code = jnp.concatenate(codes, axis=1)
        row = lax.broadcasted_iota(jnp.int32, (z.cols, 2 * LANES), 0)
        pick = (row == code).astype(jnp.float32).astype(jnp.bfloat16)
        rows = onehot_dot((parts_ref[0], parts_ref[1], parts_ref[2]), pick)
        half = lane // (z.levels * z.slots)
        for ref, at in ((tofar_ref, slice(0, LANES)), (tonear_ref, slice(LANES, 2 * LANES))):
            value = rows[0 : z.part, at]
            for h in range(1, z.halves):
                value = jnp.where(half == h, rows[h * z.part : (h + 1) * z.part, at], value)
            ref[...] = value

    copy.wait()


def final_kernel(
    z, parts_ref, far_ref, near_ref, ref_ref, src_ref, flat_ref, codes_ref, coef_ref, got_ref, turn_ref
):
    tables(z, src_ref[...], ref_ref[...], codes_ref, coef_ref)
    row = lax.broadcasted_iota(jnp.int32, (z.cols, z.cols), 0)
    pick = (row == codes_ref[0:1, :]).astype(jnp.float32).astype(jnp.bfloat16)
    own = onehot_dot((parts_ref[0], parts_ref[1], parts_ref[2]), pick)
    halo = jnp.concatenate([far_ref[...], near_ref[...]], axis=1)
    parts = split3(halo)
    row = lax.broadcasted_iota(jnp.int32, (2 * LANES, z.cols), 0)
    for h in range(z.halves):
        pick = (row == codes_ref[1 + h : 2 + h, :]).astype(jnp.float32).astype(jnp.bfloat16)
        at = slice(h * z.part, (h + 1) * z.part)
        got = own[at, :] + onehot_dot(parts, pick)
        for v in range(z.nv):
            got_ref[v, at, :] = got[:, v * LANES : (v + 1) * LANES]
    for j in range(z.tiles):
        xs, low, high = [], [], []
        for v in range(z.nv):
            x = [got_ref[v, pl.ds(j * LANES + n, z.tpt, stride=NPTS), :] for n in range(NPTS)]
            xs.append(x)
            low.append(tree(jnp.minimum, x))
            high.append(tree(jnp.maximum, x))
        for p in range(NPTS):
            coef = [coef_ref[pl.ds(n * NPTS + p, 1), :] for n in range(NPTS)]
            for v in range(z.nv):
                value = tree(jnp.add, [coef[n] * xs[v][n] for n in range(NPTS)])
                value = jnp.minimum(jnp.maximum(value, low[v]), high[v])
                turn_ref[v, pl.ds(p, z.tpt, stride=NPTS), :] = value
        for v in range(z.nv):
            block = turn_ref[v].T
            for q in range(z.per):
                level = v * z.per + q
                for e in range(0, z.elems, SUB):
                    piece = block[q * z.elems + e : q * z.elems + e + SUB, :]
                    flat_ref[j, pl.ds(e * z.levels + level, SUB, stride=z.levels), :] = piece


def scale_kernel(z, whole_weight, every_ref, mean_ref, flat_ref, out_hbm, stage_ref, sem):
    total = tree(jnp.add, [every_ref[m] for m in range(every_ref.shape[0])])
    factor = mean_ref[...] * whole_weight / total
    factor = jnp.concatenate([factor, jnp.zeros((1, LANES - z.tracers), jnp.float32)], axis=1)
    factor = jnp.broadcast_to(factor, (SUB, LANES))
    lane = lax.broadcasted_iota(jnp.int32, (SUB, LANES), 1)
    copies = []
    for j in range(z.tiles):
        mine = jnp.take_along_axis(factor, j * z.tpt + lane // NPTS, axis=1)
        stage_ref[j] = flat_ref[j] * mine[0:1, :]
        copies.append(
            pltpu.make_async_copy(
                stage_ref.at[j].reshape(z.elems, z.levels, LANES), out_hbm.at[:, :, pl.ds(j * LANES, LANES)], sem.at[j]
            )
        )
        copies[-1].start()
    for copy in copies:
        copy.wait()


def in_hbm(x):
    return pltpu.with_memory_space_constraint(x, pltpu.HBM)


def call(kernel, z, outs, ins, args, scratch=(), flops=0, nbytes=0, limit=16, spaces=None):
    return pl.pallas_call(
        functools.partial(kernel, z),
        out_shape=[jax.ShapeDtypeStruct(shape, dtype) for shape, dtype in outs],
        in_specs=[pl.BlockSpec(memory_space=space) for space in ins],
        out_specs=[pl.BlockSpec(memory_space=space) for space in spaces or [VMEM] * len(outs)],
        scratch_shapes=list(scratch),
        cost_estimate=pl.CostEstimate(flops=flops, bytes_accessed=nbytes, transcendentals=0),
        compiler_params=pltpu.CompilerParams(vmem_limit_bytes=limit << 20),
    )(*args)


def per_device(tracers, ref_index, requests, source, target_mean):
    elems, levels, width = tracers.shape
    z = Sizes(elems, levels, width, requests.shape[2])
    assert z.per == 2 and z.per * elems == LANES and z.nv * z.per == levels and z.tiles * LANES == width
    assert z.halves * levels * z.slots == LANES and z.part * z.halves == width
    f32, bf16, i32 = jnp.float32, jnp.bfloat16, jnp.int32
    flat = ((z.tiles, elems * levels, LANES), f32)
    wown, ask_far, ask_near, refs, own_source = call(
        plan_kernel, z,
        [((z.wrows, LANES), f32), ((z.wrows + SUB, LANES), f32), ((z.wrows + SUB, LANES), f32),
         ((NPTS, elems), i32), ((1, elems), i32)],
        (pltpu.HBM,) * 3, [in_hbm(a) for a in (requests, ref_index.T, source.reshape(1, elems))],
        [SMEM(requests.shape, i32), pltpu.SemaphoreType.DMA((3,))],
        flops=10**9, nbytes=10**7,
    )
    count = lax.axis_size("elem")
    assert count % 2 == 0
    far = [(i, (i - 1 if i % 2 == 0 else i + 1) % count) for i in range(count)]
    near = [(i, i + 1 if i % 2 == 0 else i - 1) for i in range(count)]
    in_far = lax.ppermute(ask_far, "elem", far)
    in_near = lax.ppermute(ask_near, "elem", near)
    parts, sums = call(
        prep_kernel, z,
        [((3, width, z.cols), bf16), ((z.wrows * z.tracers, LANES), f32)],
        (VMEM,), (tracers,), [VMEM((z.nv, width, LANES), f32)], flops=10**8, nbytes=4 * 10**6,
    )
    axes = ("elem", "lev")
    spread_shape = ((lax.axis_size(axes), 1, z.tracers), f32)
    spread, to_far, to_near = call(
        serve_kernel, z,
        [spread_shape, ((z.part, LANES), f32), ((z.part, LANES), f32)],
        (VMEM,) * 5, (wown, in_far, in_near, sums, parts),
        [VMEM((z.wrows, LANES), f32), VMEM(*spread_shape), pltpu.SemaphoreType.DMA(())],
        flops=10**7, nbytes=3 * 10**6, spaces=(pltpu.HBM, VMEM, VMEM),
    )
    from_far = lax.ppermute(to_far, "elem", far)
    from_near = lax.ppermute(to_near, "elem", near)
    every = lax.all_to_all(spread, axes, 0, 0)
    (shaped,) = call(
        final_kernel, z,
        [flat],
        (VMEM,) * 5, (parts, from_far, from_near, refs, own_source),
        [VMEM((SUB, z.cols), i32), VMEM((NPTS * NPTS, LANES), f32), VMEM((z.nv, width, LANES), f32), VMEM((z.nv, LANES, LANES), f32)],
        flops=10**8, nbytes=3 * 10**6,
    )
    whole_weight = 36.0 * 4.0 * elems * count * levels * lax.axis_size("lev")
    (out,) = call(
        lambda z, *refs: scale_kernel(z, whole_weight, *refs), z,
        [((elems, levels, width), f32)],
        (VMEM,) * 3, (every, target_mean.reshape(1, z.tracers), shaped),
        [VMEM(*flat), pltpu.SemaphoreType.DMA((z.tiles,))], flops=10**6, nbytes=10**6, spaces=(pltpu.HBM,),
    )
    return out


def solution(mesh):
    placed = (P("elem", "lev", None), P("elem", None), P("elem", None, None), P("elem"), P())

    return jax.shard_map(per_device, mesh=mesh, in_specs=placed, out_specs=P("elem", "lev", None), check_vma=False)
```

```python
import functools
import math

import jax
import jax.numpy as jnp
import numpy as np
from jax import lax
from jax.experimental import pallas as pl
from jax.experimental.pallas import tpu as pltpu
from jax.sharding import PartitionSpec as P


NPTS = 16
REFS = 64
LANES = 128
SUB = 8

VMEM = pltpu.VMEM
SMEM = pltpu.SMEM


def lagrange_1d():
    side = math.isqrt(REFS)
    nodes = [np.float32(v) for v in (-1.0, -math.sqrt(0.2), math.sqrt(0.2), 1.0)]
    points = (-1.0 + 2.0 * np.arange(side, dtype=np.float32) / np.float32(side - 1)).astype(np.float32)
    columns = []
    for which in range(4):
        basis = np.ones((side,), np.float32)
        for other in range(4):
            if other != which:
                basis = basis * (points - nodes[other]) / (nodes[which] - nodes[other])
        columns.append(basis)
    return np.stack(columns, axis=1)


SIDE = math.isqrt(REFS)
BASIS = lagrange_1d()
WEIGHT36 = [ci * cj for ci in (1, 5, 5, 1) for cj in (1, 5, 5, 1)]


def split3(x):
    a = x.astype(jnp.bfloat16)
    rest = x - a.astype(jnp.float32)
    b = rest.astype(jnp.bfloat16)
    c = (rest - b.astype(jnp.float32)).astype(jnp.bfloat16)
    return a, b, c


def onehot_dot(parts, onehot):
    return sum(jnp.dot(part, onehot, preferred_element_type=jnp.float32) for part in parts)


def mm_nt(a, b):
    return lax.dot_general(a, b, (((1,), (1,)), ((), ())), preferred_element_type=jnp.float32)


class Sizes:
    def __init__(self, elems, levels, width, slots):
        self.elems, self.levels, self.width, self.slots = elems, levels, width, slots
        self.tracers = width // NPTS
        self.per = LANES // elems
        self.nv = levels // self.per
        self.cols = levels * elems
        self.tiles = width // LANES
        self.tpt = LANES // NPTS
        self.halves = LANES // (levels * slots)
        self.part = width // self.halves
        self.wrows = REFS // self.per


def plan_kernel(
    z, req_hbm, ref_hbm, src_hbm, far_ref, note_ref, ref_ref, src_ref, req_ref, sem
):
    elems, slots = z.elems, z.slots
    copies = [
        pltpu.make_async_copy(src, dst, sem.at[i])
        for i, (src, dst) in enumerate(((req_hbm, req_ref), (ref_hbm, ref_ref), (src_hbm, src_ref)))
    ]
    for copy in copies:
        copy.start()
    odd = lax.rem(lax.axis_index("elem"), 2)
    lane = lax.broadcasted_iota(jnp.int32, (1, LANES), 1)
    k_lane = lane % slots
    for copy in copies:
        copy.wait()
    counts = count_points(z, ref_ref[...])
    src = jnp.concatenate([src_ref[...]] * z.per, axis=1)
    far_base, near_base = elems + odd * slots, elems + (1 - odd) * slots
    far = jnp.full((1, LANES), -1, jnp.int32)
    near = far
    pat_far = jnp.zeros((1, LANES), jnp.int32)
    pat_near = pat_far
    for k in range(slots):
        far_k, near_k = req_ref[0, odd, k], req_ref[0, 1 - odd, k]
        far = jnp.where(src == far_base + k, far_k, far)
        near = jnp.where(src == near_base + k, near_k, near)
        pat_far = jnp.where(k_lane == k, far_k, pat_far)
        pat_near = jnp.where(k_lane == k, near_k, pat_near)
    far_ref[0 : z.wrows, :] = weights(z, counts, far)
    far_ref[z.wrows :, :] = jnp.broadcast_to(pat_far.astype(jnp.float32), (SUB, LANES))
    note_ref[0:1, :] = near
    note_ref[1:2, :] = pat_near


def weights(z, counts, which):
    lane = lax.broadcasted_iota(jnp.int32, (1, LANES), 1)
    srow = lax.broadcasted_iota(jnp.int32, (LANES, LANES), 0)
    pick = srow == jnp.where(which >= 0, which + z.elems * (lane // z.elems), -1)
    return mm_nt(counts, pick.astype(jnp.float32).astype(jnp.bfloat16))


def count_points(z, ref):
    lane = lax.broadcasted_iota(jnp.int32, (1, LANES), 1)
    row = lax.broadcasted_iota(jnp.int32, (z.wrows, LANES), 0) + z.wrows * (lane // z.elems)
    ref = jnp.concatenate([ref] * z.per, axis=1)
    return tree(
        jnp.add, [jnp.where(row == ref[p : p + 1, :], float(WEIGHT36[p]), 0.0) for p in range(NPTS)]
    ).astype(jnp.bfloat16)


def beside_kernel(z, ref_ref, src_ref, note_ref, wown_ref, near_ref):
    counts = count_points(z, ref_ref[...])
    src = jnp.concatenate([src_ref[...]] * z.per, axis=1)
    near_ref[0 : z.wrows, :] = weights(z, counts, note_ref[0:1, :])
    near_ref[z.wrows :, :] = jnp.broadcast_to(note_ref[1:2, :].astype(jnp.float32), (SUB, LANES))
    wown_ref[...] = weights(z, counts, jnp.where(src < z.elems, src, -1))


def tables(z, src, ref, codes_ref, coef_ref):
    elems, slots, levels = z.elems, z.slots, z.levels
    odd = lax.rem(lax.axis_index("elem"), 2)
    lane = lax.broadcasted_iota(jnp.int32, (1, LANES), 1)
    src2 = jnp.concatenate([src] * z.per, axis=1)
    sub_level = lane // elems
    for v in range(z.nv):
        level = sub_level + v * z.per
        at = slice(v * LANES, (v + 1) * LANES)
        codes_ref[0:1, at] = jnp.where(src2 < elems, level * elems + src2, -1)
        rel = src2 - elems
        side = jnp.where(rel >= slots, 1, 0)
        code = jnp.where(side == odd, 0, LANES) + level * slots + (rel - side * slots)
        for h in range(z.halves):
            codes_ref[1 + h : 2 + h, at] = jnp.where(rel >= 0, code + h * levels * slots, -1)

    ref2 = jnp.concatenate([ref] * z.per, axis=1)
    one, two = ref2 // SIDE, ref2 % SIDE

    def basis(which):
        found = []
        for i in range(4):
            value = jnp.zeros(which.shape, jnp.float32)
            for a in range(SIDE):
                if BASIS[a, i] != 0.0:
                    value = jnp.where(which == a, float(BASIS[a, i]), value)
            found.append(value)
        return found

    la, lb = basis(one), basis(two)
    for i in range(4):
        for j in range(4):
            n = 4 * i + j
            coef_ref[n * NPTS : (n + 1) * NPTS, :] = la[i] * lb[j]


def line(x):
    out = [None] * SIDE
    out[0], out[SIDE - 1] = x[0], x[3]
    outer, inner = x[0] + x[3], x[1] + x[2]
    outer_odd, inner_odd = x[0] - x[3], x[1] - x[2]
    for a in range(1, SIDE // 2):
        c = [float(v) for v in BASIS[a]]
        even = (0.5 * (c[0] + c[3])) * outer + (0.5 * (c[1] + c[2])) * inner
        odd = (0.5 * (c[0] - c[3])) * outer_odd + (0.5 * (c[1] - c[2])) * inner_odd
        out[a], out[SIDE - 1 - a] = even + odd, even - odd
    return out


def tree(op, values):
    while len(values) > 1:
        values = [op(values[i], values[i + 1]) if i + 1 < len(values) else values[i] for i in range(0, len(values), 2)]
    return values[0]


def prep_kernel(z, x_ref, parts_ref, sums_ref, xt_ref):
    for j in range(z.tiles):
        for v in range(z.nv):
            rows = []
            for q in range(z.per):
                level = v * z.per + q
                for e in range(0, z.elems, SUB):
                    rows.append(x_ref[pl.ds(e, SUB), level, pl.ds(j * LANES, LANES)])
            block = jnp.concatenate(rows, axis=0)
            xt_ref[v, j * LANES : (j + 1) * LANES, :] = block.T
    a, b, c = split3(jnp.concatenate([xt_ref[v] for v in range(z.nv)], axis=1))
    parts_ref[0], parts_ref[1], parts_ref[2] = a, b, c
    for j in range(z.tiles):
        both = [None] * REFS
        for v in range(z.nv):
            x = [xt_ref[v, pl.ds(j * LANES + n, z.tpt, stride=NPTS), :] for n in range(NPTS)]
            lowest, highest = tree(jnp.minimum, x), tree(jnp.maximum, x)
            lines = [line(x[4 * i : 4 * i + 4]) for i in range(4)]
            for b in range(SIDE):
                column = line([lines[i][b] for i in range(4)])
                for a in range(SIDE):
                    value = jnp.minimum(jnp.maximum(column[a], lowest), highest)
                    r = a * SIDE + b
                    both[r] = value if both[r] is None else both[r] + value
        low = lax.broadcasted_iota(jnp.int32, (1, LANES), 1) < z.elems
        for r in range(z.wrows):
            one, two = both[r], both[r + z.wrows]
            folded = jnp.where(low, one, two) + pltpu.roll(jnp.where(low, two, one), z.elems, 1)
            sums_ref[r * z.tracers + j * z.tpt : r * z.tracers + (j + 1) * z.tpt, :] = folded


def serve_kernel(
    z, wown_ref, infar_ref, innear_ref, sums_ref, parts_ref, spread_hbm, tofar_ref, tonear_ref, weight_ref, mass_ref, sem
):
    weight_ref[...] = wown_ref[...] + infar_ref[0 : z.wrows, :] + innear_ref[0 : z.wrows, :]
    terms = [[] for _ in range(z.tiles)]
    for r in range(z.wrows):
        w = weight_ref[pl.ds(r, 1), :]
        for j in range(z.tiles):
            lo = r * z.tracers + j * z.tpt
            term = sums_ref[lo : lo + z.tpt, :] * w
            if len(terms[j]) < 4:
                terms[j].append(term)
            else:
                terms[j][r % 4] = terms[j][r % 4] + term
    total = jnp.concatenate([tree(jnp.add, parts) for parts in terms], axis=0)
    mass = jnp.sum(total.T, axis=0, keepdims=True)
    mass_ref[...] = jnp.broadcast_to(mass[None], mass_ref.shape)
    copy = pltpu.make_async_copy(mass_ref, spread_hbm, sem)
    copy.start()

    @pl.when(lax.axis_index("elem") >= 0)
    def _():
        lane = lax.broadcasted_iota(jnp.int32, (1, LANES), 1)
        level = (lane // z.slots) % z.levels
        codes = []
        for ref in (infar_ref, innear_ref):
            wanted = ref[z.wrows : z.wrows + 1, :].astype(jnp.int32)
            codes.append(jnp.where(wanted >= 0, level * z.elems + wanted, -1))
        code = jnp.concatenate(codes, axis=1)
        row = lax.broadcasted_iota(jnp.int32, (z.cols, 2 * LANES), 0)
        pick = (row == code).astype(jnp.float32).astype(jnp.bfloat16)
        rows = onehot_dot((parts_ref[0], parts_ref[1], parts_ref[2]), pick)
        half = lane // (z.levels * z.slots)
        for ref, at in ((tofar_ref, slice(0, LANES)), (tonear_ref, slice(LANES, 2 * LANES))):
            value = rows[0 : z.part, at]
            for h in range(1, z.halves):
                value = jnp.where(half == h, rows[h * z.part : (h + 1) * z.part, at], value)
            ref[...] = value

    copy.wait()


def final_kernel(
    z, parts_ref, far_ref, near_ref, ref_ref, src_ref, flat_ref, codes_ref, coef_ref, got_ref, turn_ref
):
    tables(z, src_ref[...], ref_ref[...], codes_ref, coef_ref)
    row = lax.broadcasted_iota(jnp.int32, (z.cols, z.cols), 0)
    pick = (row == codes_ref[0:1, :]).astype(jnp.float32).astype(jnp.bfloat16)
    own = onehot_dot((parts_ref[0], parts_ref[1], parts_ref[2]), pick)
    halo = jnp.concatenate([far_ref[...], near_ref[...]], axis=1)
    parts = split3(halo)
    row = lax.broadcasted_iota(jnp.int32, (2 * LANES, z.cols), 0)
    for h in range(z.halves):
        pick = (row == codes_ref[1 + h : 2 + h, :]).astype(jnp.float32).astype(jnp.bfloat16)
        at = slice(h * z.part, (h + 1) * z.part)
        got = own[at, :] + onehot_dot(parts, pick)
        for v in range(z.nv):
            got_ref[v, at, :] = got[:, v * LANES : (v + 1) * LANES]
    for j in range(z.tiles):
        xs, low, high = [], [], []
        for v in range(z.nv):
            x = [got_ref[v, pl.ds(j * LANES + n, z.tpt, stride=NPTS), :] for n in range(NPTS)]
            xs.append(x)
            low.append(tree(jnp.minimum, x))
            high.append(tree(jnp.maximum, x))
        for p in range(NPTS):
            coef = [coef_ref[pl.ds(n * NPTS + p, 1), :] for n in range(NPTS)]
            for v in range(z.nv):
                value = tree(jnp.add, [coef[n] * xs[v][n] for n in range(NPTS)])
                value = jnp.minimum(jnp.maximum(value, low[v]), high[v])
                turn_ref[v, pl.ds(p, z.tpt, stride=NPTS), :] = value
        for v in range(z.nv):
            block = turn_ref[v].T
            for q in range(z.per):
                level = v * z.per + q
                for e in range(0, z.elems, SUB):
                    piece = block[q * z.elems + e : q * z.elems + e + SUB, :]
                    flat_ref[j, pl.ds(e * z.levels + level, SUB, stride=z.levels), :] = piece


def scale_kernel(z, whole_weight, every_ref, mean_ref, flat_ref, out_hbm, stage_ref, sem):
    total = tree(jnp.add, [every_ref[m] for m in range(every_ref.shape[0])])
    factor = mean_ref[...] * whole_weight / total
    factor = jnp.concatenate([factor, jnp.zeros((1, LANES - z.tracers), jnp.float32)], axis=1)
    factor = jnp.broadcast_to(factor, (SUB, LANES))
    lane = lax.broadcasted_iota(jnp.int32, (SUB, LANES), 1)
    copies = []
    for j in range(z.tiles):
        mine = jnp.take_along_axis(factor, j * z.tpt + lane // NPTS, axis=1)
        stage_ref[j] = flat_ref[j] * mine[0:1, :]
        copies.append(
            pltpu.make_async_copy(
                stage_ref.at[j].reshape(z.elems, z.levels, LANES), out_hbm.at[:, :, pl.ds(j * LANES, LANES)], sem.at[j]
            )
        )
        copies[-1].start()
    for copy in copies:
        copy.wait()


def in_hbm(x):
    return pltpu.with_memory_space_constraint(x, pltpu.HBM)


def call(kernel, z, outs, ins, args, scratch=(), flops=0, nbytes=0, limit=16, spaces=None):
    return pl.pallas_call(
        functools.partial(kernel, z),
        out_shape=[jax.ShapeDtypeStruct(shape, dtype) for shape, dtype in outs],
        in_specs=[pl.BlockSpec(memory_space=space) for space in ins],
        out_specs=[pl.BlockSpec(memory_space=space) for space in spaces or [VMEM] * len(outs)],
        scratch_shapes=list(scratch),
        cost_estimate=pl.CostEstimate(flops=flops, bytes_accessed=nbytes, transcendentals=0),
        compiler_params=pltpu.CompilerParams(vmem_limit_bytes=limit << 20),
    )(*args)


def per_device(tracers, ref_index, requests, source, target_mean):
    elems, levels, width = tracers.shape
    z = Sizes(elems, levels, width, requests.shape[2])
    assert z.per == 2 and z.per * elems == LANES and z.nv * z.per == levels and z.tiles * LANES == width
    assert z.halves * levels * z.slots == LANES and z.part * z.halves == width
    f32, bf16, i32 = jnp.float32, jnp.bfloat16, jnp.int32
    flat = ((z.tiles, elems * levels, LANES), f32)
    far_ask, note, refs, own_source = call(
        plan_kernel, z,
        [((z.wrows + SUB, LANES), f32), ((SUB, LANES), i32), ((NPTS, elems), i32), ((1, elems), i32)],
        (pltpu.HBM,) * 3, [in_hbm(a) for a in (requests, ref_index.T, source.reshape(1, elems))],
        [SMEM(requests.shape, i32), pltpu.SemaphoreType.DMA((3,))],
        flops=10**9, nbytes=10**7,
    )
    wown, ask_near = call(
        beside_kernel, z,
        [((z.wrows, LANES), f32), ((z.wrows + SUB, LANES), f32)],
        (VMEM,) * 3, (refs, own_source, note), flops=10**6, nbytes=10**5,
    )
    count = lax.axis_size("elem")
    assert count % 2 == 0
    far = [(i, (i - 1 if i % 2 == 0 else i + 1) % count) for i in range(count)]
    near = [(i, i + 1 if i % 2 == 0 else i - 1) for i in range(count)]
    in_far = lax.ppermute(far_ask, "elem", far)
    in_near = lax.ppermute(ask_near, "elem", near)
    parts, sums = call(
        prep_kernel, z,
        [((3, width, z.cols), bf16), ((z.wrows * z.tracers, LANES), f32)],
        (VMEM,), (tracers,), [VMEM((z.nv, width, LANES), f32)], flops=10**8, nbytes=4 * 10**6,
    )
    axes = ("elem", "lev")
    spread_shape = ((lax.axis_size(axes), 1, z.tracers), f32)
    spread, to_far, to_near = call(
        serve_kernel, z,
        [spread_shape, ((z.part, LANES), f32), ((z.part, LANES), f32)],
        (VMEM,) * 5, (wown, in_far, in_near, sums, parts),
        [VMEM((z.wrows, LANES), f32), VMEM(*spread_shape), pltpu.SemaphoreType.DMA(())],
        flops=10**7, nbytes=3 * 10**6, spaces=(pltpu.HBM, VMEM, VMEM),
    )
    from_far = lax.ppermute(to_far, "elem", far)
    from_near = lax.ppermute(to_near, "elem", near)
    every = lax.all_to_all(spread, axes, 0, 0)
    (shaped,) = call(
        final_kernel, z,
        [flat],
        (VMEM,) * 5, (parts, from_far, from_near, refs, own_source),
        [VMEM((SUB, z.cols), i32), VMEM((NPTS * NPTS, LANES), f32), VMEM((z.nv, width, LANES), f32), VMEM((z.nv, LANES, LANES), f32)],
        flops=10**8, nbytes=3 * 10**6,
    )
    whole_weight = 36.0 * 4.0 * elems * count * levels * lax.axis_size("lev")
    (out,) = call(
        lambda z, *refs: scale_kernel(z, whole_weight, *refs), z,
        [((elems, levels, width), f32)],
        (VMEM,) * 3, (every, target_mean.reshape(1, z.tracers), shaped),
        [VMEM(*flat), pltpu.SemaphoreType.DMA((z.tiles,))], flops=10**6, nbytes=10**6, spaces=(pltpu.HBM,),
    )
    return out


def solution(mesh):
    placed = (P("elem", "lev", None), P("elem", None), P("elem", None, None), P("elem"), P())

    return jax.shard_map(per_device, mesh=mesh, in_specs=placed, out_specs=P("elem", "lev", None), check_vma=False)
```

```python
import functools
import math

import jax
import jax.numpy as jnp
import numpy as np
from jax import lax
from jax.experimental import pallas as pl
from jax.experimental.pallas import tpu as pltpu
from jax.sharding import PartitionSpec as P


NPTS = 16
REFS = 64
LANES = 128
SUB = 8

VMEM = pltpu.VMEM
SMEM = pltpu.SMEM


def lagrange_1d():
    side = math.isqrt(REFS)
    nodes = [np.float32(v) for v in (-1.0, -math.sqrt(0.2), math.sqrt(0.2), 1.0)]
    points = (-1.0 + 2.0 * np.arange(side, dtype=np.float32) / np.float32(side - 1)).astype(np.float32)
    columns = []
    for which in range(4):
        basis = np.ones((side,), np.float32)
        for other in range(4):
            if other != which:
                basis = basis * (points - nodes[other]) / (nodes[which] - nodes[other])
        columns.append(basis)
    return np.stack(columns, axis=1)


SIDE = math.isqrt(REFS)
BASIS = lagrange_1d()
WEIGHT36 = [ci * cj for ci in (1, 5, 5, 1) for cj in (1, 5, 5, 1)]


def split3(x):
    a = x.astype(jnp.bfloat16)
    rest = x - a.astype(jnp.float32)
    b = rest.astype(jnp.bfloat16)
    c = (rest - b.astype(jnp.float32)).astype(jnp.bfloat16)
    return a, b, c


def onehot_dot(parts, onehot):
    return sum(jnp.dot(part, onehot, preferred_element_type=jnp.float32) for part in parts)


def mm_nt(a, b):
    return lax.dot_general(a, b, (((1,), (1,)), ((), ())), preferred_element_type=jnp.float32)


class Sizes:
    def __init__(self, elems, levels, width, slots):
        self.elems, self.levels, self.width, self.slots = elems, levels, width, slots
        self.tracers = width // NPTS
        self.per = LANES // elems
        self.nv = levels // self.per
        self.cols = levels * elems
        self.tiles = width // LANES
        self.tpt = LANES // NPTS
        self.halves = LANES // (levels * slots)
        self.part = width // self.halves
        self.wrows = REFS // self.per


def plan_kernel(
    z, req_hbm, ref_hbm, src_hbm, wown_ref, far_ref, near_ref, ref_ref, src_ref, req_ref, sem
):
    elems, slots = z.elems, z.slots
    copies = [
        pltpu.make_async_copy(src, dst, sem.at[i])
        for i, (src, dst) in enumerate(((req_hbm, req_ref), (ref_hbm, ref_ref), (src_hbm, src_ref)))
    ]
    for copy in copies:
        copy.start()
    odd = lax.rem(lax.axis_index("elem"), 2)
    lane = lax.broadcasted_iota(jnp.int32, (1, LANES), 1)
    group = lane // elems
    row = lax.broadcasted_iota(jnp.int32, (z.wrows, LANES), 0) + z.wrows * group
    srow = lax.broadcasted_iota(jnp.int32, (LANES, LANES), 0)
    k_lane = lane % slots
    for copy in copies:
        copy.wait()
    ref = jnp.concatenate([ref_ref[...]] * z.per, axis=1)
    counts = tree(jnp.add, [jnp.where(row == ref[p : p + 1, :], float(WEIGHT36[p]), 0.0) for p in range(NPTS)])
    counts = counts.astype(jnp.bfloat16)
    src = jnp.concatenate([src_ref[...]] * z.per, axis=1)
    far_base, near_base = elems + odd * slots, elems + (1 - odd) * slots
    far = jnp.full((1, LANES), -1, jnp.int32)
    near = far
    pat_far = jnp.zeros((1, LANES), jnp.int32)
    pat_near = pat_far
    for k in range(slots):
        far_k, near_k = req_ref[0, odd, k], req_ref[0, 1 - odd, k]
        far = jnp.where(src == far_base + k, far_k, far)
        near = jnp.where(src == near_base + k, near_k, near)
        pat_far = jnp.where(k_lane == k, far_k, pat_far)
        pat_near = jnp.where(k_lane == k, near_k, pat_near)
    own = jnp.where(src < elems, src, -1)

    def weights(which):
        pick = srow == jnp.where(which >= 0, which + elems * group, -1)
        return mm_nt(counts, pick.astype(jnp.float32).astype(jnp.bfloat16))

    far_ref[0 : z.wrows, :] = weights(far)
    far_ref[z.wrows :, :] = jnp.broadcast_to(pat_far.astype(jnp.float32), (SUB, LANES))
    near_ref[0 : z.wrows, :] = weights(near)
    near_ref[z.wrows :, :] = jnp.broadcast_to(pat_near.astype(jnp.float32), (SUB, LANES))
    wown_ref[...] = weights(own)


def tables(z, src, ref, codes_ref, coef_ref):
    elems, slots, levels = z.elems, z.slots, z.levels
    odd = lax.rem(lax.axis_index("elem"), 2)
    lane = lax.broadcasted_iota(jnp.int32, (1, LANES), 1)
    src2 = jnp.concatenate([src] * z.per, axis=1)
    sub_level = lane // elems
    for v in range(z.nv):
        level = sub_level + v * z.per
        at = slice(v * LANES, (v + 1) * LANES)
        codes_ref[0:1, at] = jnp.where(src2 < elems, level * elems + src2, -1)
        rel = src2 - elems
        side = jnp.where(rel >= slots, 1, 0)
        code = jnp.where(side == odd, 0, LANES) + level * slots + (rel - side * slots)
        for h in range(z.halves):
            codes_ref[1 + h : 2 + h, at] = jnp.where(rel >= 0, code + h * levels * slots, -1)

    ref2 = jnp.concatenate([ref] * z.per, axis=1)
    one, two = ref2 // SIDE, ref2 % SIDE

    def basis(which):
        found = []
        for i in range(4):
            value = jnp.zeros(which.shape, jnp.float32)
            for a in range(SIDE):
                if BASIS[a, i] != 0.0:
                    value = jnp.where(which == a, float(BASIS[a, i]), value)
            found.append(value)
        return found

    la, lb = basis(one), basis(two)
    for i in range(4):
        for j in range(4):
            n = 4 * i + j
            coef_ref[n * NPTS : (n + 1) * NPTS, :] = la[i] * lb[j]


def line(x):
    out = [None] * SIDE
    out[0], out[SIDE - 1] = x[0], x[3]
    outer, inner = x[0] + x[3], x[1] + x[2]
    outer_odd, inner_odd = x[0] - x[3], x[1] - x[2]
    for a in range(1, SIDE // 2):
        c = [float(v) for v in BASIS[a]]
        even = (0.5 * (c[0] + c[3])) * outer + (0.5 * (c[1] + c[2])) * inner
        odd = (0.5 * (c[0] - c[3])) * outer_odd + (0.5 * (c[1] - c[2])) * inner_odd
        out[a], out[SIDE - 1 - a] = even + odd, even - odd
    return out


def tree(op, values):
    while len(values) > 1:
        values = [op(values[i], values[i + 1]) if i + 1 < len(values) else values[i] for i in range(0, len(values), 2)]
    return values[0]


def prep_kernel(z, x_ref, parts_ref, sums_ref, xt_ref):
    for j in range(z.tiles):
        for v in range(z.nv):
            rows = []
            for q in range(z.per):
                level = v * z.per + q
                for e in range(0, z.elems, SUB):
                    rows.append(x_ref[pl.ds(e, SUB), level, pl.ds(j * LANES, LANES)])
            block = jnp.concatenate(rows, axis=0)
            xt_ref[v, j * LANES : (j + 1) * LANES, :] = block.T
    a, b, c = split3(jnp.concatenate([xt_ref[v] for v in range(z.nv)], axis=1))
    parts_ref[0], parts_ref[1], parts_ref[2] = a, b, c
    for j in range(z.tiles):
        both = [None] * REFS
        for v in range(z.nv):
            x = [xt_ref[v, pl.ds(j * LANES + n, z.tpt, stride=NPTS), :] for n in range(NPTS)]
            lowest, highest = tree(jnp.minimum, x), tree(jnp.maximum, x)
            lines = [line(x[4 * i : 4 * i + 4]) for i in range(4)]
            for b in range(SIDE):
                column = line([lines[i][b] for i in range(4)])
                for a in range(SIDE):
                    value = jnp.minimum(jnp.maximum(column[a], lowest), highest)
                    r = a * SIDE + b
                    both[r] = value if both[r] is None else both[r] + value
        low = lax.broadcasted_iota(jnp.int32, (1, LANES), 1) < z.elems
        for r in range(z.wrows):
            one, two = both[r], both[r + z.wrows]
            folded = jnp.where(low, one, two) + pltpu.roll(jnp.where(low, two, one), z.elems, 1)
            sums_ref[r * z.tracers + j * z.tpt : r * z.tracers + (j + 1) * z.tpt, :] = folded


def serve_kernel(
    z, wown_ref, infar_ref, innear_ref, sums_ref, parts_ref, spread_hbm, tofar_ref, tonear_ref, mass_ref, sem
):
    weight = wown_ref[...] + infar_ref[0 : z.wrows, :] + innear_ref[0 : z.wrows, :]
    terms = [[] for _ in range(z.tiles)]
    for r in range(z.wrows):
        w = weight[r : r + 1, :]
        for j in range(z.tiles):
            lo = r * z.tracers + j * z.tpt
            term = sums_ref[lo : lo + z.tpt, :] * w
            if len(terms[j]) < 4:
                terms[j].append(term)
            else:
                terms[j][r % 4] = terms[j][r % 4] + term
    total = jnp.concatenate([tree(jnp.add, parts) for parts in terms], axis=0)
    mass = jnp.sum(total.T, axis=0, keepdims=True)
    mass_ref[...] = jnp.broadcast_to(mass[None], mass_ref.shape)
    copy = pltpu.make_async_copy(mass_ref, spread_hbm, sem)
    copy.start()

    @pl.when(lax.axis_index("elem") >= 0)
    def _():
        lane = lax.broadcasted_iota(jnp.int32, (1, LANES), 1)
        level = (lane // z.slots) % z.levels
        codes = []
        for ref in (infar_ref, innear_ref):
            wanted = ref[z.wrows : z.wrows + 1, :].astype(jnp.int32)
            codes.append(jnp.where(wanted >= 0, level * z.elems + wanted, -1))
        code = jnp.concatenate(codes, axis=1)
        row = lax.broadcasted_iota(jnp.int32, (z.cols, 2 * LANES), 0)
        pick = (row == code).astype(jnp.float32).astype(jnp.bfloat16)
        rows = onehot_dot((parts_ref[0], parts_ref[1], parts_ref[2]), pick)
        half = lane // (z.levels * z.slots)
        for ref, at in ((tofar_ref, slice(0, LANES)), (tonear_ref, slice(LANES, 2 * LANES))):
            value = rows[0 : z.part, at]
            for h in range(1, z.halves):
                value = jnp.where(half == h, rows[h * z.part : (h + 1) * z.part, at], value)
            ref[...] = value

    copy.wait()


def final_kernel(
    z, parts_ref, far_ref, near_ref, ref_ref, src_ref, flat_ref, codes_ref, coef_ref, got_ref, turn_ref
):
    tables(z, src_ref[...], ref_ref[...], codes_ref, coef_ref)
    row = lax.broadcasted_iota(jnp.int32, (z.cols, z.cols), 0)
    pick = (row == codes_ref[0:1, :]).astype(jnp.float32).astype(jnp.bfloat16)
    own = onehot_dot((parts_ref[0], parts_ref[1], parts_ref[2]), pick)
    halo = jnp.concatenate([far_ref[...], near_ref[...]], axis=1)
    parts = split3(halo)
    row = lax.broadcasted_iota(jnp.int32, (2 * LANES, z.cols), 0)
    for h in range(z.halves):
        pick = (row == codes_ref[1 + h : 2 + h, :]).astype(jnp.float32).astype(jnp.bfloat16)
        at = slice(h * z.part, (h + 1) * z.part)
        got = own[at, :] + onehot_dot(parts, pick)
        for v in range(z.nv):
            got_ref[v, at, :] = got[:, v * LANES : (v + 1) * LANES]
    for j in range(z.tiles):
        xs, low, high = [], [], []
        for v in range(z.nv):
            x = [got_ref[v, pl.ds(j * LANES + n, z.tpt, stride=NPTS), :] for n in range(NPTS)]
            xs.append(x)
            low.append(tree(jnp.minimum, x))
            high.append(tree(jnp.maximum, x))
        for p in range(NPTS):
            coef = [coef_ref[pl.ds(n * NPTS + p, 1), :] for n in range(NPTS)]
            for v in range(z.nv):
                value = tree(jnp.add, [coef[n] * xs[v][n] for n in range(NPTS)])
                value = jnp.minimum(jnp.maximum(value, low[v]), high[v])
                turn_ref[v, pl.ds(p, z.tpt, stride=NPTS), :] = value
        for v in range(z.nv):
            block = turn_ref[v].T
            for q in range(z.per):
                level = v * z.per + q
                for e in range(0, z.elems, SUB):
                    piece = block[q * z.elems + e : q * z.elems + e + SUB, :]
                    flat_ref[j, pl.ds(e * z.levels + level, SUB, stride=z.levels), :] = piece


def scale_kernel(z, whole_weight, every_ref, mean_ref, flat_ref, out_hbm, stage_ref, sem):
    total = tree(jnp.add, [every_ref[m] for m in range(every_ref.shape[0])])
    factor = mean_ref[...] * whole_weight / total
    factor = jnp.concatenate([factor, jnp.zeros((1, LANES - z.tracers), jnp.float32)], axis=1)
    factor = jnp.broadcast_to(factor, (SUB, LANES))
    lane = lax.broadcasted_iota(jnp.int32, (SUB, LANES), 1)
    copies = []
    for j in range(z.tiles):
        mine = jnp.take_along_axis(factor, j * z.tpt + lane // NPTS, axis=1)
        stage_ref[j] = flat_ref[j] * mine[0:1, :]
        copies.append(
            pltpu.make_async_copy(
                stage_ref.at[j].reshape(z.elems, z.levels, LANES), out_hbm.at[:, :, pl.ds(j * LANES, LANES)], sem.at[j]
            )
        )
        copies[-1].start()
    for copy in copies:
        copy.wait()


def in_hbm(x):
    return pltpu.with_memory_space_constraint(x, pltpu.HBM)


def call(kernel, z, outs, ins, args, scratch=(), flops=0, nbytes=0, limit=16, spaces=None):
    return pl.pallas_call(
        functools.partial(kernel, z),
        out_shape=[jax.ShapeDtypeStruct(shape, dtype) for shape, dtype in outs],
        in_specs=[pl.BlockSpec(memory_space=space) for space in ins],
        out_specs=[pl.BlockSpec(memory_space=space) for space in spaces or [VMEM] * len(outs)],
        scratch_shapes=list(scratch),
        cost_estimate=pl.CostEstimate(flops=flops, bytes_accessed=nbytes, transcendentals=0),
        compiler_params=pltpu.CompilerParams(vmem_limit_bytes=limit << 20),
    )(*args)


def per_device(tracers, ref_index, requests, source, target_mean):
    elems, levels, width = tracers.shape
    z = Sizes(elems, levels, width, requests.shape[2])
    assert z.per == 2 and z.per * elems == LANES and z.nv * z.per == levels and z.tiles * LANES == width
    assert z.halves * levels * z.slots == LANES and z.part * z.halves == width
    f32, bf16, i32 = jnp.float32, jnp.bfloat16, jnp.int32
    flat = ((z.tiles, elems * levels, LANES), f32)
    wown, ask_far, ask_near, refs, own_source = call(
        plan_kernel, z,
        [((z.wrows, LANES), f32), ((z.wrows + SUB, LANES), f32), ((z.wrows + SUB, LANES), f32),
         ((NPTS, elems), i32), ((1, elems), i32)],
        (pltpu.HBM,) * 3, [in_hbm(a) for a in (requests, ref_index.T, source.reshape(1, elems))],
        [SMEM(requests.shape, i32), pltpu.SemaphoreType.DMA((3,))],
        flops=10**9, nbytes=10**7,
    )
    count = lax.axis_size("elem")
    assert count % 2 == 0
    far = [(i, (i - 1 if i % 2 == 0 else i + 1) % count) for i in range(count)]
    near = [(i, i + 1 if i % 2 == 0 else i - 1) for i in range(count)]
    in_far = lax.ppermute(ask_far, "elem", far)
    in_near = lax.ppermute(ask_near, "elem", near)
    parts, sums = call(
        prep_kernel, z,
        [((3, width, z.cols), bf16), ((z.wrows * z.tracers, LANES), f32)],
        (VMEM,), (tracers,), [VMEM((z.nv, width, LANES), f32)], flops=10**8, nbytes=4 * 10**6,
    )
    axes = ("elem", "lev")
    spread_shape = ((lax.axis_size(axes), 1, z.tracers), f32)
    spread, to_far, to_near = call(
        serve_kernel, z,
        [spread_shape, ((z.part, LANES), f32), ((z.part, LANES), f32)],
        (VMEM,) * 5, (wown, in_far, in_near, sums, parts),
        [VMEM(*spread_shape), pltpu.SemaphoreType.DMA(())],
        flops=10**7, nbytes=3 * 10**6, spaces=(pltpu.HBM, VMEM, VMEM),
    )
    from_far = lax.ppermute(to_far, "elem", far)
    from_near = lax.ppermute(to_near, "elem", near)
    every = lax.all_to_all(spread, axes, 0, 0)
    (shaped,) = call(
        final_kernel, z,
        [flat],
        (VMEM,) * 5, (parts, from_far, from_near, refs, own_source),
        [VMEM((SUB, z.cols), i32), VMEM((NPTS * NPTS, LANES), f32), VMEM((z.nv, width, LANES), f32), VMEM((z.nv, LANES, LANES), f32)],
        flops=10**8, nbytes=3 * 10**6,
    )
    whole_weight = 36.0 * 4.0 * elems * count * levels * lax.axis_size("lev")
    (out,) = call(
        lambda z, *refs: scale_kernel(z, whole_weight, *refs), z,
        [((elems, levels, width), f32)],
        (VMEM,) * 3, (every, target_mean.reshape(1, z.tracers), shaped),
        [VMEM(*flat), pltpu.SemaphoreType.DMA((z.tiles,))], flops=10**6, nbytes=10**6, spaces=(pltpu.HBM,),
    )
    return out


def solution(mesh):
    placed = (P("elem", "lev", None), P("elem", None), P("elem", None, None), P("elem"), P())

    return jax.shard_map(per_device, mesh=mesh, in_specs=placed, out_specs=P("elem", "lev", None), check_vma=False)
```
